128 devices in a mesh: row: 8 (over z_lo, y), col: 16 (over z_hi, x, core).
Axes of the slice: x: 4, y: 4, z: 4 (z_hi: 2, z_lo: 2; z = z_hi * 2 + z_lo), core: 2. Of those that a mesh axis runs over, the one named last changes fastest.
Arguments:
- initial_field: float32 [256, 256, 256], P(('row', 'col')), may hold values from -5 to 5
Outputs:
- advanced_field: float32 [256, 256, 256], P(('row', 'col'))
The draws below stay inside these ranges and needn't reach their ends.
All inputs are finite; a program needn't handle non-finite values.
Results may differ from the reference program's by a relative error of at most 0.0003.
Values sent between devices are 32-bit elements; how exact they have to be, the bound alone decides.
No kernel may reach another device: no remote copies, remote signals or barrier semaphores. Data moves between devices by JAX's collectives and lax.ppermute only.
A program may use at most 64 MiB of HBM per device.

```python
import math
import jax
import jax.numpy as jnp

NX = 256
NY = 256
NZ = 256


def level_of(stream_key, dims, split, least, high):
    def one(position, blocks):
        heights = jax.random.uniform(jax.random.fold_in(jax.random.fold_in(stream_key, 6), position), (blocks,), jnp.float32, least / len(split), high / len(split))
        return jnp.repeat(jnp.exp(heights), dims[position] // blocks).reshape((-1,) + (1,) * (len(dims) - position - 1))

    gain = one(*split[0])
    for cut in split[1:]:
        gain = gain * one(*cut)
    return gain


def noise(own_key, dims, scale, bound, split=(), dtype=jnp.bfloat16):
    result = scale * jax.random.normal(own_key, dims, jnp.float32)
    if split:
        result = result * level_of(own_key, dims, split, -0.22, 0.18)
    return jnp.clip(result, -bound, bound).astype(dtype)


def setup_inputs(seed: int = 0) -> dict:
    key_of = jax.random.split(jax.random.key(seed), 2)
    initial_field = noise(key_of[0], (NX, NY, NZ), 1.0, 5.0, ((0, 128),), jnp.float32)
    return dict(initial_field=initial_field)


growth_rate = 0.3
quadratic = 1.0
time_step = 0.2
wave_scale = 4.0


def wavenumbers(count, offset, length):
    indices = (offset + jnp.arange(count)).astype(jnp.int32)
    signed = jnp.where(indices * 2 < length, indices, indices - length)
    return wave_scale * signed.astype(jnp.float32) / length


def phi_values(argument):
    within = jnp.abs(argument) < 1.0
    inside = jnp.where(within, argument, 0.0)
    outside = jnp.where(within, 2.0, argument)
    series = []
    for degree in (1, 2, 3):
        running = jnp.zeros_like(argument) + 1.0 / math.factorial(11 + degree)
        for exponent in range(10, -1, -1):
            running = running * inside + 1.0 / math.factorial(exponent + degree)
        series.append(running)
    growth_term = jnp.exp(outside)
    closed_one = (growth_term - 1.0) / outside
    closed_two = (growth_term - 1.0 - outside) / (outside * outside)
    closed_three = (growth_term - 1.0 - outside - 0.5 * outside * outside) / (outside * outside * outside)
    return (jnp.where(within, series[0], closed_one), jnp.where(within, series[1], closed_two), jnp.where(within, series[2], closed_three))


def step_factors(ksq):
    lin = growth_rate - (1.0 - ksq) * (1.0 - ksq)
    scaled = time_step * lin
    half_phi, _, _ = phi_values(0.5 * scaled)
    first_phi, second_phi, third_phi = phi_values(scaled)
    e_half = jnp.exp(0.5 * scaled)
    q_half = 0.5 * time_step * half_phi
    e_full = jnp.exp(scaled)
    f_one = time_step * (first_phi - 3.0 * second_phi + 4.0 * third_phi)
    f_two = time_step * (second_phi - 2.0 * third_phi)
    f_three = time_step * (4.0 * third_phi - second_phi)
    return e_half, q_half, e_full, f_one, f_two, f_three


def reaction(values):
    return quadratic * values * values - values * values * values


def reference(initial_field):
    wave_x = wavenumbers(NX, 0, NX)
    wave_y = wavenumbers(NY, 0, NY)
    wave_z = wavenumbers(NZ, 0, NZ)
    ksq = wave_x[:, None, None] ** 2 + wave_y[None, :, None] ** 2 + wave_z[None, None, :] ** 2
    e_half, q_half, e_full, f_one, f_two, f_three = step_factors(ksq)

    def forward_fft(values):
        return jnp.fft.fftn(values)

    def inverse_fft(spectrum):
        return jnp.fft.ifftn(spectrum).real

    state_hat = forward_fft(initial_field)
    react_u = forward_fft(reaction(initial_field))
    first_hat = e_half * state_hat + q_half * react_u
    react_a = forward_fft(reaction(inverse_fft(first_hat)))
    second_hat = e_half * state_hat + q_half * react_a
    react_b = forward_fft(reaction(inverse_fft(second_hat)))
    third_hat = e_half * first_hat + q_half * (2.0 * react_b - react_u)
    react_c = forward_fft(reaction(inverse_fft(third_hat)))
    new_hat = e_full * state_hat + f_one * react_u + 2.0 * f_two * (react_a + react_b) + f_three * react_c
    return inverse_fft(new_hat).astype(jnp.float32)
```

```python
import functools
import math

import jax
import jax.numpy as jnp
import numpy as np
from jax import lax
from jax.experimental import pallas as pl
from jax.experimental.pallas import tpu as pltpu
from jax.sharding import PartitionSpec as P

growth_rate = 0.3
quadratic = 1.0
time_step = 0.2
wave_scale = 4.0

N = 256
H = 128
BOTH = ("row", "col")
F32 = jnp.float32
BF16 = jnp.bfloat16


def tables():
    n = np.arange(N)
    j = np.arange(H)
    angle = 2.0 * np.pi / N * ((j[:, None] * n[None, :]) % N)
    cosine = np.cos(angle)
    sine = np.sin(angle)
    alternate = 1.0 - 2.0 * (n % 2)
    sine_alt = sine.copy()
    sine_alt[0] = alternate
    forward_y = np.concatenate([cosine, sine_alt])
    inverse_y = forward_y.T / N
    order = np.concatenate([np.arange(0, N, 2), np.arange(1, N, 2)])
    forward_x = forward_y[:, order]
    inverse_x = inverse_y[order]
    minus = -sine
    minus[0] = alternate
    forward_z = np.concatenate([cosine, minus]).T
    weight = np.where(j == 0, 1.0, 2.0)[:, None] / N
    inverse_z = np.concatenate([cosine * weight, minus * weight])
    return dict(fx=forward_x, ix=inverse_x, fy=forward_y, iy=inverse_y, fz=forward_z, iz=inverse_z)


def split_table(table):
    high = np.asarray(table, np.float32).astype(jnp.bfloat16)
    low = (table - high.astype(np.float64)).astype(np.float32).astype(jnp.bfloat16)
    return np.stack([high, low])


def split(values):
    high = values.astype(BF16)
    low = (values - high.astype(F32)).astype(BF16)
    return high, low


def dot(left, right):
    return jnp.dot(left, right, preferred_element_type=F32)


def table_left(table, values):
    high, low = split(values)
    return dot(table[0], high) + (dot(table[0], low) + dot(table[1], high))


def table_right(values, table):
    high, low = split(values)
    return dot(high, table[0]) + (dot(low, table[0]) + dot(high, table[1]))


def grid_of(axis):
    return lax.broadcasted_iota(jnp.int32, (H, H), axis)


def quarters(whole):
    return whole[:H, :H], whole[:H, H:], whole[H:, :H], whole[H:, H:]


def joined(top_left, top_right, bottom_left, bottom_right):
    return jnp.concatenate(
        [
            jnp.concatenate([top_left, top_right], axis=1),
            jnp.concatenate([bottom_left, bottom_right], axis=1),
        ],
        axis=0,
    )


def tile_rows(ref, slot):
    return ref[pl.ds(slot, H, stride=ref.shape[0] // H), :]


def put_rows(ref, slot, values):
    ref[pl.ds(slot, H, stride=ref.shape[0] // H), :] = values


def reaction(values):
    return quadratic * values * values - values * values * values


def send_modes(whole, send, base):
    cre, cim, sre, sim = quarters(whole)
    lane0 = grid_of(1) == 0
    row0 = grid_of(0) == 0
    corner = lane0 & row0
    o0re = jnp.where(lane0 | row0, cre, cre + sim)
    o0im = jnp.where(lane0, -sre, cim - sre)
    o0im = jnp.where(row0, cim, o0im)
    o0im = jnp.where(corner, sim, o0im)
    o1re = jnp.where(row0, sre, cre - sim)
    o1re = jnp.where(lane0, cim, o1re)
    o1im = jnp.where(lane0, -sim, cim + sre)
    o1im = jnp.where(row0, sim, o1im)
    o1im = jnp.where(corner, sre, o1im)
    put_rows(send, base + 0, o0re)
    put_rows(send, base + 1, o0im)
    put_rows(send, base + 2, o1re)
    put_rows(send, base + 3, o1im)


def got_modes(got, base):
    s0re = tile_rows(got, base + 0)
    s0im = tile_rows(got, base + 1)
    s1re = tile_rows(got, base + 2)
    s1im = tile_rows(got, base + 3)
    lane0 = grid_of(1) == 0
    row0 = grid_of(0) == 0
    corner = lane0 & row0
    pre = jnp.where(lane0, 2.0 * s0re, s0re + s1re)
    pre = jnp.where(row0, s0re, pre)
    pim = jnp.where(lane0, 2.0 * s1re, s0im + s1im)
    pim = jnp.where(row0, s0im, pim)
    pim = jnp.where(corner, s1re, pim)
    mre = jnp.where(lane0, -2.0 * s0im, s1im - s0im)
    mre = jnp.where(row0, s1re, mre)
    mre = jnp.where(corner, s1im, mre)
    mim = jnp.where(lane0, -2.0 * s1im, s0re - s1re)
    mim = jnp.where(row0, s1im, mim)
    mim = jnp.where(corner, s0im, mim)
    return joined(pre, pim, mre, mim)


def from_messages(got, base, iy, iz):
    modes = got_modes(got, base)
    half = table_left(iy, modes)
    return table_right(half, iz)


def to_messages(values, send, base, fz, fy):
    half = table_right(values, fz)
    send_modes(table_left(fy, half), send, base)


def first_kernel(field, fz, fy, send):
    for row in range(2):
        values = field[row]
        to_messages(values, send, 4 * row, fz, fy)
        to_messages(reaction(values), send, 8 + 4 * row, fz, fy)


def middle_kernel(got, iy, iz, fz, fy, send):
    for row in range(2):
        values = from_messages(got, 4 * row, iy, iz)
        to_messages(reaction(values), send, 4 * row, fz, fy)


def last_kernel(got, iy, iz, field):
    for row in range(2):
        field[row] = from_messages(got, 4 * row, iy, iz)


def special_lane(slot):
    if slot:
        return None
    device = lax.axis_index(BOTH)
    lane = grid_of(1) + jnp.where(device == 0, 0, H)
    return (lane == 0) & (grid_of(0) != 0)


def spectrum_of(got, slot, fx, field=0):
    at = 8 * field + 2 * slot
    column = joined(*(tile_rows(got, at + k) for k in (0, 1, 4, 5)))
    cre, cim, sre, sim = quarters(table_left(fx, column))
    row0 = grid_of(0) == 0
    tre = jnp.where(row0, cre, cre + sim)
    tim = jnp.where(row0, cim, cim - sre)
    bre = jnp.where(row0, sre, cre - sim)
    bim = jnp.where(row0, sim, cim + sre)
    special = special_lane(slot)
    if special is not None:
        tre = jnp.where(special, cre, tre)
        tim = jnp.where(special, -sre, tim)
        bre = jnp.where(special, cim, bre)
        bim = jnp.where(special, -sim, bim)
    return tre, tim, bre, bim


def spectrum_to(parts, slot, ix, send):
    tre, tim, bre, bim = parts
    row0 = grid_of(0) == 0
    pre = jnp.where(row0, tre, tre + bre)
    pim = jnp.where(row0, tim, tim + bim)
    mre = jnp.where(row0, bre, bim - tim)
    mim = jnp.where(row0, bim, tre - bre)
    special = special_lane(slot)
    if special is not None:
        pre = jnp.where(special, 2.0 * tre, pre)
        pim = jnp.where(special, 2.0 * bre, pim)
        mre = jnp.where(special, -2.0 * tim, mre)
        mim = jnp.where(special, -2.0 * bim, mim)
    out = table_left(ix, joined(pre, pim, mre, mim))
    a, b, c, d = quarters(out)
    put_rows(send, 2 * slot, a)
    put_rows(send, 2 * slot + 1, b)
    put_rows(send, 2 * slot + 4, c)
    put_rows(send, 2 * slot + 5, d)


def plane_of(slot, half, part):
    if slot:
        return 2 + half
    return (4 if part else 0) + half


def each_part():
    for half in range(2):
        for part in range(2):
            yield 2 * half + part, half, part


def spectral_first(got, factors, fx, ix, send, keep, base, total):
    for slot in range(2):
        state = spectrum_of(got, slot, fx)
        react = spectrum_of(got, slot, fx, field=1)
        nexts = []
        for k, half, part in each_part():
            plane = plane_of(slot, half, part)
            e_half = factors[0, plane]
            q_half = factors[1, plane]
            kept = e_half * state[k]
            turn = q_half * react[k]
            first = kept + turn
            keep[4 * slot + k] = kept
            base[4 * slot + k] = e_half * first - turn
            total[4 * slot + k] = factors[2, plane] * state[k] + factors[3, plane] * react[k]
            nexts.append(first)
        spectrum_to(nexts, slot, ix, send)


def spectral_middle(got, factors, kept, total, fx, ix, send, total_out, *, twice):
    for slot in range(2):
        react = spectrum_of(got, slot, fx)
        nexts = []
        for k, half, part in each_part():
            plane = plane_of(slot, half, part)
            turn = factors[1, plane] * react[k]
            if twice:
                turn = 2.0 * turn
            nexts.append(kept[4 * slot + k] + turn)
            total_out[4 * slot + k] = total[4 * slot + k] + 2.0 * factors[4, plane] * react[k]
        spectrum_to(nexts, slot, ix, send)


def spectral_last(got, factors, total, fx, ix, send):
    for slot in range(2):
        react = spectrum_of(got, slot, fx)
        nexts = []
        for k, half, part in each_part():
            plane = plane_of(slot, half, part)
            nexts.append(total[4 * slot + k] + factors[5, plane] * react[k])
        spectrum_to(nexts, slot, ix, send)


def phi_values(argument, degrees):
    within = jnp.abs(argument) < 1.0
    inside = jnp.where(within, argument, 0.0)
    outside = jnp.where(within, 2.0, argument)
    series = []
    for degree in degrees:
        running = jnp.zeros_like(argument) + 1.0 / math.factorial(11 + degree)
        for exponent in range(10, -1, -1):
            running = running * inside + 1.0 / math.factorial(exponent + degree)
        series.append(running)
    growth = jnp.exp(outside)
    closed = [(growth - 1.0) / outside]
    if len(degrees) > 1:
        square = outside * outside
        closed.append((growth - 1.0 - outside) / square)
        closed.append((growth - 1.0 - outside - 0.5 * square) / (square * outside))
    return [jnp.where(within, s, c) for s, c in zip(series, closed)]


def factor_kernel(factors):
    device = lax.axis_index(BOTH)
    square = H * H
    row = grid_of(0)
    lane = grid_of(1)
    own = device * device
    alone = jnp.where(device == 0, 1, 0)
    for plane in range(6):
        half = plane % 2
        slot = 1 if plane // 2 == 1 else 0
        imaginary = plane // 2 == 2
        modes = row * row
        if half:
            modes = jnp.where(row == 0, square, modes)
        lane0 = lane == 0
        if slot:
            modes = modes + own + alone * square
            modes = modes + jnp.where(lane0, (1 - alone) * square, lane * lane)
        else:
            modes = modes + own + lane * lane
            pair = lane0 & (row == 0) if not half else (lane0 & (row != 0))
            if imaginary and half:
                pair = lane0
            if half or imaginary:
                modes = modes + jnp.where(pair, alone * (2 * square), 0)
        ksq = modes.astype(F32) * (wave_scale / N) ** 2
        lin = growth_rate - (1.0 - ksq) * (1.0 - ksq)
        scaled = time_step * lin
        (half_phi,) = phi_values(0.5 * scaled, (1,))
        first, second, third = phi_values(scaled, (1, 2, 3))
        factors[0, plane] = jnp.exp(0.5 * scaled)
        factors[1, plane] = 0.5 * time_step * half_phi
        factors[2, plane] = jnp.exp(scaled)
        factors[3, plane] = time_step * (first - 3.0 * second + 4.0 * third)
        factors[4, plane] = time_step * (second - 2.0 * third)
        factors[5, plane] = time_step * (4.0 * third - second)


def shape(*dims):
    return jax.ShapeDtypeStruct(dims, F32)


def call(kernel, outs, *args, name):
    vmem = pl.BlockSpec(memory_space=pltpu.VMEM)
    single = not isinstance(outs, tuple)
    return pl.pallas_call(
        kernel,
        out_shape=outs,
        in_specs=[vmem] * len(args),
        out_specs=vmem if single else tuple(vmem for _ in outs),
        name=name,
    )(*args)


def move(send):
    tiles = send.reshape(H, send.shape[0] // H, H)
    out = lax.all_to_all(tiles, BOTH, split_axis=0, concat_axis=0, tiled=True)
    return out.reshape(send.shape)


def body(tabs, field):
    fx, ix, fy, iy, fz, iz = (tabs[k] for k in ("fx", "ix", "fy", "iy", "fz", "iz"))
    message = shape(8 * H, H)
    spectrum = shape(8, H, H)
    factors = call(factor_kernel, shape(6, 6, H, H), name="factors")
    send = call(first_kernel, shape(16 * H, H), field, fz, fy, name="first")
    got = move(send)
    send, keep, base, total = call(
        spectral_first, (message, spectrum, spectrum, spectrum), got, factors, fx, ix, name="spectral_first"
    )

    def physical(send):
        return move(call(middle_kernel, message, move(send), iy, iz, fz, fy, name="physical"))

    for kept, twice in ((keep, False), (base, True)):
        got = physical(send)
        send, total = call(
            functools.partial(spectral_middle, twice=twice),
            (message, spectrum),
            got, factors, kept, total, fx, ix,
            name="spectral_middle",
        )
    got = physical(send)
    send = call(spectral_last, message, got, factors, total, fx, ix, name="spectral_last")
    return call(last_kernel, shape(2, N, N), move(send), iy, iz, name="last")


def solution(mesh):
    tabs = {k: split_table(v) for k, v in tables().items()}
    placed = P(BOTH, None, None)

    def run(initial_field):
        return body({k: jnp.asarray(v) for k, v in tabs.items()}, initial_field)

    return jax.shard_map(run, mesh=mesh, in_specs=(placed,), out_specs=placed, check_vma=False)
```

```python
import functools
import math

import jax
import jax.numpy as jnp
import numpy as np
from jax import lax
from jax.experimental import pallas as pl
from jax.experimental.pallas import tpu as pltpu
from jax.sharding import PartitionSpec as P

growth_rate = 0.3
quadratic = 1.0
time_step = 0.2
wave_scale = 4.0

N = 256
H = 128
BOTH = ("row", "col")
F32 = jnp.float32
BF16 = jnp.bfloat16


def tables():
    n = np.arange(N)
    j = np.arange(H)
    angle = 2.0 * np.pi / N * ((j[:, None] * n[None, :]) % N)
    cosine = np.cos(angle)
    sine = np.sin(angle)
    alternate = 1.0 - 2.0 * (n % 2)
    sine_alt = sine.copy()
    sine_alt[0] = alternate
    forward_y = np.concatenate([cosine, sine_alt])
    inverse_y = forward_y.T / N
    order = np.concatenate([np.arange(0, N, 2), np.arange(1, N, 2)])
    forward_x = forward_y[:, order]
    inverse_x = inverse_y[order]
    minus = -sine
    minus[0] = alternate
    forward_z = np.concatenate([cosine, minus]).T
    weight = np.where(j == 0, 1.0, 2.0)[:, None] / N
    inverse_z = np.concatenate([cosine * weight, minus * weight])
    return dict(fx=forward_x, ix=inverse_x, fy=forward_y, iy=inverse_y, fz=forward_z, iz=inverse_z)


def split_table(table):
    high = np.asarray(table, np.float32).astype(jnp.bfloat16)
    low = (table - high.astype(np.float64)).astype(np.float32).astype(jnp.bfloat16)
    return np.stack([high, low])


def split(values):
    high = values.astype(BF16)
    low = (values - high.astype(F32)).astype(BF16)
    return high, low


def dot(left, right):
    return jnp.dot(left, right, preferred_element_type=F32)


def table_left(table, values):
    high, low = split(values)
    return dot(table[0], high) + (dot(table[0], low) + dot(table[1], high))


def table_right(values, table):
    high, low = split(values)
    return dot(high, table[0]) + (dot(low, table[0]) + dot(high, table[1]))


def grid_of(axis):
    return lax.broadcasted_iota(jnp.int32, (H, H), axis)


def quarters(whole):
    return whole[:H, :H], whole[:H, H:], whole[H:, :H], whole[H:, H:]


def joined(top_left, top_right, bottom_left, bottom_right):
    return jnp.concatenate(
        [
            jnp.concatenate([top_left, top_right], axis=1),
            jnp.concatenate([bottom_left, bottom_right], axis=1),
        ],
        axis=0,
    )


def tile_rows(ref, slot):
    return ref[pl.ds(slot, H, stride=ref.shape[0] // H), :]


def put_rows(ref, slot, values):
    ref[pl.ds(slot, H, stride=ref.shape[0] // H), :] = values


def reaction(values):
    return quadratic * values * values - values * values * values


def send_modes(whole, send, base):
    cre, cim, sre, sim = quarters(whole)
    lane0 = grid_of(1) == 0
    row0 = grid_of(0) == 0
    corner = lane0 & row0
    o0re = jnp.where(lane0 | row0, cre, cre + sim)
    o0im = jnp.where(lane0, -sre, cim - sre)
    o0im = jnp.where(row0, cim, o0im)
    o0im = jnp.where(corner, sim, o0im)
    o1re = jnp.where(row0, sre, cre - sim)
    o1re = jnp.where(lane0, cim, o1re)
    o1im = jnp.where(lane0, -sim, cim + sre)
    o1im = jnp.where(row0, sim, o1im)
    o1im = jnp.where(corner, sre, o1im)
    put_rows(send, base + 0, o0re)
    put_rows(send, base + 1, o0im)
    put_rows(send, base + 2, o1re)
    put_rows(send, base + 3, o1im)


def got_modes(got, base):
    s0re = tile_rows(got, base + 0)
    s0im = tile_rows(got, base + 1)
    s1re = tile_rows(got, base + 2)
    s1im = tile_rows(got, base + 3)
    lane0 = grid_of(1) == 0
    row0 = grid_of(0) == 0
    corner = lane0 & row0
    pre = jnp.where(lane0, 2.0 * s0re, s0re + s1re)
    pre = jnp.where(row0, s0re, pre)
    pim = jnp.where(lane0, 2.0 * s1re, s0im + s1im)
    pim = jnp.where(row0, s0im, pim)
    pim = jnp.where(corner, s1re, pim)
    mre = jnp.where(lane0, -2.0 * s0im, s1im - s0im)
    mre = jnp.where(row0, s1re, mre)
    mre = jnp.where(corner, s1im, mre)
    mim = jnp.where(lane0, -2.0 * s1im, s0re - s1re)
    mim = jnp.where(row0, s1im, mim)
    mim = jnp.where(corner, s0im, mim)
    return joined(pre, pim, mre, mim)


def from_messages(got, base, iy, iz):
    modes = got_modes(got, base)
    half = table_left(iy, modes)
    return table_right(half, iz)


def to_messages(values, send, base, fz, fy):
    half = table_right(values, fz)
    send_modes(table_left(fy, half), send, base)


def first_kernel(field, fz, fy, send):
    for row in range(2):
        values = field[row]
        to_messages(values, send, 4 * row, fz, fy)
        to_messages(reaction(values), send, 8 + 4 * row, fz, fy)


def middle_kernel(got, iy, iz, fz, fy, send):
    for row in range(2):
        values = from_messages(got, 4 * row, iy, iz)
        to_messages(reaction(values), send, 4 * row, fz, fy)


def last_kernel(got, iy, iz, field):
    for row in range(2):
        field[row] = from_messages(got, 4 * row, iy, iz)


def special_lane(slot):
    if slot:
        return None
    device = lax.axis_index(BOTH)
    lane = grid_of(1) + jnp.where(device == 0, 0, H)
    return (lane == 0) & (grid_of(0) != 0)


def spectrum_of(got, slot, fx, field=0):
    at = 8 * field + 2 * slot
    column = joined(*(tile_rows(got, at + k) for k in (0, 1, 4, 5)))
    cre, cim, sre, sim = quarters(table_left(fx, column))
    row0 = grid_of(0) == 0
    tre = jnp.where(row0, cre, cre + sim)
    tim = jnp.where(row0, cim, cim - sre)
    bre = jnp.where(row0, sre, cre - sim)
    bim = jnp.where(row0, sim, cim + sre)
    special = special_lane(slot)
    if special is not None:
        tre = jnp.where(special, cre, tre)
        tim = jnp.where(special, -sre, tim)
        bre = jnp.where(special, cim, bre)
        bim = jnp.where(special, -sim, bim)
    return tre, tim, bre, bim


def spectrum_to(parts, slot, ix, send):
    tre, tim, bre, bim = parts
    row0 = grid_of(0) == 0
    pre = jnp.where(row0, tre, tre + bre)
    pim = jnp.where(row0, tim, tim + bim)
    mre = jnp.where(row0, bre, bim - tim)
    mim = jnp.where(row0, bim, tre - bre)
    special = special_lane(slot)
    if special is not None:
        pre = jnp.where(special, 2.0 * tre, pre)
        pim = jnp.where(special, 2.0 * bre, pim)
        mre = jnp.where(special, -2.0 * tim, mre)
        mim = jnp.where(special, -2.0 * bim, mim)
    out = table_left(ix, joined(pre, pim, mre, mim))
    a, b, c, d = quarters(out)
    put_rows(send, 2 * slot, a)
    put_rows(send, 2 * slot + 1, b)
    put_rows(send, 2 * slot + 4, c)
    put_rows(send, 2 * slot + 5, d)


def plane_of(slot, half, part):
    if slot:
        return 2 + half
    return (4 if part else 0) + half


def each_part():
    for half in range(2):
        for part in range(2):
            yield 2 * half + part, half, part


def spectral_first(got, factors, fx, ix, send, keep, base, total):
    for slot in range(2):
        state = spectrum_of(got, slot, fx)
        react = spectrum_of(got, slot, fx, field=1)
        nexts = []
        for k, half, part in each_part():
            plane = plane_of(slot, half, part)
            e_half = factors[0, plane]
            q_half = factors[1, plane]
            kept = e_half * state[k]
            turn = q_half * react[k]
            first = kept + turn
            keep[4 * slot + k] = kept
            base[4 * slot + k] = e_half * first - turn
            total[4 * slot + k] = factors[2, plane] * state[k] + factors[3, plane] * react[k]
            nexts.append(first)
        spectrum_to(nexts, slot, ix, send)


def spectral_middle(got, factors, kept, total, fx, ix, send, total_out, *, twice):
    for slot in range(2):
        react = spectrum_of(got, slot, fx)
        nexts = []
        for k, half, part in each_part():
            plane = plane_of(slot, half, part)
            turn = factors[1, plane] * react[k]
            if twice:
                turn = 2.0 * turn
            nexts.append(kept[4 * slot + k] + turn)
            total_out[4 * slot + k] = total[4 * slot + k] + 2.0 * factors[4, plane] * react[k]
        spectrum_to(nexts, slot, ix, send)


def spectral_last(got, factors, total, fx, ix, send):
    for slot in range(2):
        react = spectrum_of(got, slot, fx)
        nexts = []
        for k, half, part in each_part():
            plane = plane_of(slot, half, part)
            nexts.append(total[4 * slot + k] + factors[5, plane] * react[k])
        spectrum_to(nexts, slot, ix, send)


def phi_values(argument, degrees):
    within = jnp.abs(argument) < 1.0
    inside = jnp.where(within, argument, 0.0)
    outside = jnp.where(within, 2.0, argument)
    series = []
    for degree in degrees:
        running = jnp.zeros_like(argument) + 1.0 / math.factorial(11 + degree)
        for exponent in range(10, -1, -1):
            running = running * inside + 1.0 / math.factorial(exponent + degree)
        series.append(running)
    growth = jnp.exp(outside)
    closed = [(growth - 1.0) / outside]
    if len(degrees) > 1:
        square = outside * outside
        closed.append((growth - 1.0 - outside) / square)
        closed.append((growth - 1.0 - outside - 0.5 * square) / (square * outside))
    return [jnp.where(within, s, c) for s, c in zip(series, closed)]


def factor_kernel(factors):
    device = lax.axis_index(BOTH)
    square = H * H
    row = grid_of(0)
    lane = grid_of(1)
    own = device * device
    alone = jnp.where(device == 0, 1, 0)
    for plane in range(6):
        half = plane % 2
        slot = 1 if plane // 2 == 1 else 0
        imaginary = plane // 2 == 2
        modes = row * row
        if half:
            modes = jnp.where(row == 0, square, modes)
        lane0 = lane == 0
        if slot:
            modes = modes + own + alone * square
            modes = modes + jnp.where(lane0, (1 - alone) * square, lane * lane)
        else:
            modes = modes + own + lane * lane
            pair = lane0 & (row == 0) if not half else (lane0 & (row != 0))
            if imaginary and half:
                pair = lane0
            if half or imaginary:
                modes = modes + jnp.where(pair, alone * (2 * square), 0)
        ksq = modes.astype(F32) * (wave_scale / N) ** 2
        lin = growth_rate - (1.0 - ksq) * (1.0 - ksq)
        scaled = time_step * lin
        (half_phi,) = phi_values(0.5 * scaled, (1,))
        first, second, third = phi_values(scaled, (1, 2, 3))
        factors[0, plane] = jnp.exp(0.5 * scaled)
        factors[1, plane] = 0.5 * time_step * half_phi
        factors[2, plane] = jnp.exp(scaled)
        factors[3, plane] = time_step * (first - 3.0 * second + 4.0 * third)
        factors[4, plane] = time_step * (second - 2.0 * third)
        factors[5, plane] = time_step * (4.0 * third - second)


def shape(*dims):
    return jax.ShapeDtypeStruct(dims, F32)


def call(kernel, outs, *args, name):
    vmem = pl.BlockSpec(memory_space=pltpu.VMEM)
    single = not isinstance(outs, tuple)
    return pl.pallas_call(
        kernel,
        out_shape=outs,
        in_specs=[vmem] * len(args),
        out_specs=vmem if single else tuple(vmem for _ in outs),
        compiler_params=pltpu.CompilerParams(vmem_limit_bytes=16 << 20),
        name=name,
    )(*args)


def move(send):
    tiles = send.reshape(H, send.shape[0] // H, H)
    out = lax.all_to_all(tiles, BOTH, split_axis=0, concat_axis=0, tiled=True)
    return out.reshape(send.shape)


def body(tabs, field):
    fx, ix, fy, iy, fz, iz = (tabs[k] for k in ("fx", "ix", "fy", "iy", "fz", "iz"))
    message = shape(8 * H, H)
    spectrum = shape(8, H, H)
    factors = call(factor_kernel, shape(6, 6, H, H), name="factors")
    send = call(first_kernel, shape(16 * H, H), field, fz, fy, name="first")
    got = move(send)
    send, keep, base, total = call(
        spectral_first, (message, spectrum, spectrum, spectrum), got, factors, fx, ix, name="spectral_first"
    )

    def physical(send):
        return move(call(middle_kernel, message, move(send), iy, iz, fz, fy, name="physical"))

    for kept, twice in ((keep, False), (base, True)):
        got = physical(send)
        send, total = call(
            functools.partial(spectral_middle, twice=twice),
            (message, spectrum),
            got, factors, kept, total, fx, ix,
            name="spectral_middle",
        )
    got = physical(send)
    send = call(spectral_last, message, got, factors, total, fx, ix, name="spectral_last")
    return call(last_kernel, shape(2, N, N), move(send), iy, iz, name="last")


def solution(mesh):
    tabs = {k: split_table(v) for k, v in tables().items()}
    placed = P(BOTH, None, None)

    def run(initial_field):
        return body({k: jnp.asarray(v) for k, v in tabs.items()}, initial_field)

    return jax.shard_map(run, mesh=mesh, in_specs=(placed,), out_specs=placed, check_vma=False)
```

```python
import functools
import math

import jax
import jax.numpy as jnp
import numpy as np
from jax import lax
from jax.experimental import pallas as pl
from jax.experimental.pallas import tpu as pltpu
from jax.sharding import PartitionSpec as P

growth_rate = 0.3
quadratic = 1.0
time_step = 0.2
wave_scale = 4.0

N = 256
H = 128
BOTH = ("row", "col")
F32 = jnp.float32
BF16 = jnp.bfloat16


def tables():
    n = np.arange(N)
    j = np.arange(H)
    angle = 2.0 * np.pi / N * ((j[:, None] * n[None, :]) % N)
    cosine = np.cos(angle)
    sine = np.sin(angle)
    alternate = 1.0 - 2.0 * (n % 2)
    sine_alt = sine.copy()
    sine_alt[0] = alternate
    forward_y = np.concatenate([cosine, sine_alt])
    inverse_y = forward_y.T / N
    order = np.concatenate([np.arange(0, N, 2), np.arange(1, N, 2)])
    forward_x = forward_y[:, order]
    inverse_x = inverse_y[order]
    minus = -sine
    minus[0] = alternate
    forward_z = np.concatenate([cosine, minus]).T
    weight = np.where(j == 0, 1.0, 2.0)[:, None] / N
    inverse_z = np.concatenate([cosine * weight, minus * weight])
    return forward_z, forward_y, forward_x, inverse_x, inverse_y, inverse_z


FZ, FY, FX, IX, IY, IZ = range(6)


def split_table(table):
    high = np.asarray(table, np.float32).astype(jnp.bfloat16)
    low = (table - high.astype(np.float64)).astype(np.float32).astype(jnp.bfloat16)
    return np.stack([high, low])


def split(values):
    high = values.astype(BF16)
    low = (values - high.astype(F32)).astype(BF16)
    return high, low


def dot(left, right):
    return jnp.dot(left, right, preferred_element_type=F32)


def table_left(table, values):
    high, low = split(values)
    return dot(table[0], high) + (dot(table[0], low) + dot(table[1], high))


def table_right(values, table):
    high, low = split(values)
    return dot(high, table[0]) + (dot(low, table[0]) + dot(high, table[1]))


def grid_of(axis):
    return lax.broadcasted_iota(jnp.int32, (H, H), axis)


def quarters(whole):
    return whole[:H, :H], whole[:H, H:], whole[H:, :H], whole[H:, H:]


def joined(top_left, top_right, bottom_left, bottom_right):
    return jnp.concatenate(
        [
            jnp.concatenate([top_left, top_right], axis=1),
            jnp.concatenate([bottom_left, bottom_right], axis=1),
        ],
        axis=0,
    )


def tile_rows(ref, slot):
    return ref[pl.ds(slot, H, stride=ref.shape[0] // H), :]


def put_rows(ref, slot, values):
    ref[pl.ds(slot, H, stride=ref.shape[0] // H), :] = values


def reaction(values):
    return quadratic * values * values - values * values * values


def send_modes(whole, send, base):
    cre, cim, sre, sim = quarters(whole)
    lane0 = grid_of(1) == 0
    row0 = grid_of(0) == 0
    corner = lane0 & row0
    o0re = jnp.where(lane0 | row0, cre, cre + sim)
    o0im = jnp.where(lane0, -sre, cim - sre)
    o0im = jnp.where(row0, cim, o0im)
    o0im = jnp.where(corner, sim, o0im)
    o1re = jnp.where(row0, sre, cre - sim)
    o1re = jnp.where(lane0, cim, o1re)
    o1im = jnp.where(lane0, -sim, cim + sre)
    o1im = jnp.where(row0, sim, o1im)
    o1im = jnp.where(corner, sre, o1im)
    put_rows(send, base + 0, o0re)
    put_rows(send, base + 1, o0im)
    put_rows(send, base + 2, o1re)
    put_rows(send, base + 3, o1im)


def got_modes(got, base):
    s0re = tile_rows(got, base + 0)
    s0im = tile_rows(got, base + 1)
    s1re = tile_rows(got, base + 2)
    s1im = tile_rows(got, base + 3)
    lane0 = grid_of(1) == 0
    row0 = grid_of(0) == 0
    corner = lane0 & row0
    pre = jnp.where(lane0, 2.0 * s0re, s0re + s1re)
    pre = jnp.where(row0, s0re, pre)
    pim = jnp.where(lane0, 2.0 * s1re, s0im + s1im)
    pim = jnp.where(row0, s0im, pim)
    pim = jnp.where(corner, s1re, pim)
    mre = jnp.where(lane0, -2.0 * s0im, s1im - s0im)
    mre = jnp.where(row0, s1re, mre)
    mre = jnp.where(corner, s1im, mre)
    mim = jnp.where(lane0, -2.0 * s1im, s0re - s1re)
    mim = jnp.where(row0, s1im, mim)
    mim = jnp.where(corner, s0im, mim)
    return joined(pre, pim, mre, mim)


def from_messages(got, base, iy, iz):
    modes = got_modes(got, base)
    half = table_left(iy, modes)
    return table_right(half, iz)


def to_messages(values, send, base, fz, fy):
    half = table_right(values, fz)
    send_modes(table_left(fy, half), send, base)


def first_kernel(field_hbm, tabs_hbm, send, factors, tabs, field, sems):
    def load(source, target, at):
        return pltpu.make_async_copy(source, target, sems.at[at])

    own = load(field_hbm, field, 0)
    loads = [load(tabs_hbm.at[k], tabs.at[k], 1 + k) for k in range(6)]
    own.start()
    for one in loads:
        one.start()
    factor_kernel(factors)
    own.wait()
    loads[FZ].wait()
    loads[FY].wait()
    fz, fy = tabs.at[FZ], tabs.at[FY]
    for row in range(2):
        values = field[row]
        to_messages(values, send, 4 * row, fz, fy)
        to_messages(reaction(values), send, 8 + 4 * row, fz, fy)
    for k in (FX, IX, IY, IZ):
        loads[k].wait()


def middle_kernel(got, tabs, send):
    fz, fy, iy, iz = (tabs.at[k] for k in (FZ, FY, IY, IZ))
    for row in range(2):
        values = from_messages(got, 4 * row, iy, iz)
        to_messages(reaction(values), send, 4 * row, fz, fy)


def last_kernel(got, tabs, field_hbm, field, sems):
    stores = []
    for row in range(2):
        field[row] = from_messages(got, 4 * row, tabs.at[IY], tabs.at[IZ])
        one = pltpu.make_async_copy(field.at[row], field_hbm.at[row], sems.at[row])
        one.start()
        stores.append(one)
    for one in stores:
        one.wait()


def special_lane(slot):
    if slot:
        return None
    device = lax.axis_index(BOTH)
    lane = grid_of(1) + jnp.where(device == 0, 0, H)
    return (lane == 0) & (grid_of(0) != 0)


def spectrum_of(got, slot, fx, field=0):
    at = 8 * field + 2 * slot
    column = joined(*(tile_rows(got, at + k) for k in (0, 1, 4, 5)))
    cre, cim, sre, sim = quarters(table_left(fx, column))
    row0 = grid_of(0) == 0
    tre = jnp.where(row0, cre, cre + sim)
    tim = jnp.where(row0, cim, cim - sre)
    bre = jnp.where(row0, sre, cre - sim)
    bim = jnp.where(row0, sim, cim + sre)
    special = special_lane(slot)
    if special is not None:
        tre = jnp.where(special, cre, tre)
        tim = jnp.where(special, -sre, tim)
        bre = jnp.where(special, cim, bre)
        bim = jnp.where(special, -sim, bim)
    return tre, tim, bre, bim


def spectrum_to(parts, slot, ix, send):
    tre, tim, bre, bim = parts
    row0 = grid_of(0) == 0
    pre = jnp.where(row0, tre, tre + bre)
    pim = jnp.where(row0, tim, tim + bim)
    mre = jnp.where(row0, bre, bim - tim)
    mim = jnp.where(row0, bim, tre - bre)
    special = special_lane(slot)
    if special is not None:
        pre = jnp.where(special, 2.0 * tre, pre)
        pim = jnp.where(special, 2.0 * bre, pim)
        mre = jnp.where(special, -2.0 * tim, mre)
        mim = jnp.where(special, -2.0 * bim, mim)
    out = table_left(ix, joined(pre, pim, mre, mim))
    a, b, c, d = quarters(out)
    put_rows(send, 2 * slot, a)
    put_rows(send, 2 * slot + 1, b)
    put_rows(send, 2 * slot + 4, c)
    put_rows(send, 2 * slot + 5, d)


def plane_of(slot, half, part):
    if slot:
        return 2 + half
    return (4 if part else 0) + half


def each_part():
    for half in range(2):
        for part in range(2):
            yield 2 * half + part, half, part


def spectral_first(got, factors, tabs, send, keep, base, total):
    fx, ix = tabs.at[FX], tabs.at[IX]
    for slot in range(2):
        state = spectrum_of(got, slot, fx)
        react = spectrum_of(got, slot, fx, field=1)
        nexts = []
        for k, half, part in each_part():
            plane = plane_of(slot, half, part)
            e_half = factors[0, plane]
            q_half = factors[1, plane]
            kept = e_half * state[k]
            turn = q_half * react[k]
            first = kept + turn
            keep[4 * slot + k] = kept
            base[4 * slot + k] = e_half * first - turn
            total[4 * slot + k] = factors[2, plane] * state[k] + factors[3, plane] * react[k]
            nexts.append(first)
        spectrum_to(nexts, slot, ix, send)


def spectral_middle(got, factors, kept, total, tabs, send, total_out, *, twice):
    fx, ix = tabs.at[FX], tabs.at[IX]
    for slot in range(2):
        react = spectrum_of(got, slot, fx)
        nexts = []
        for k, half, part in each_part():
            plane = plane_of(slot, half, part)
            turn = factors[1, plane] * react[k]
            if twice:
                turn = 2.0 * turn
            nexts.append(kept[4 * slot + k] + turn)
            total_out[4 * slot + k] = total[4 * slot + k] + 2.0 * factors[4, plane] * react[k]
        spectrum_to(nexts, slot, ix, send)


def spectral_last(got, factors, total, tabs, send):
    fx, ix = tabs.at[FX], tabs.at[IX]
    for slot in range(2):
        react = spectrum_of(got, slot, fx)
        nexts = []
        for k, half, part in each_part():
            plane = plane_of(slot, half, part)
            nexts.append(total[4 * slot + k] + factors[5, plane] * react[k])
        spectrum_to(nexts, slot, ix, send)


def phi_values(argument, degrees):
    within = jnp.abs(argument) < 1.0
    inside = jnp.where(within, argument, 0.0)
    outside = jnp.where(within, 2.0, argument)
    series = []
    for degree in degrees:
        running = jnp.zeros_like(argument) + 1.0 / math.factorial(11 + degree)
        for exponent in range(10, -1, -1):
            running = running * inside + 1.0 / math.factorial(exponent + degree)
        series.append(running)
    growth = jnp.exp(outside)
    closed = [(growth - 1.0) / outside]
    if len(degrees) > 1:
        square = outside * outside
        closed.append((growth - 1.0 - outside) / square)
        closed.append((growth - 1.0 - outside - 0.5 * square) / (square * outside))
    return [jnp.where(within, s, c) for s, c in zip(series, closed)]


def factor_kernel(factors):
    device = lax.axis_index(BOTH)
    square = H * H
    row = grid_of(0)
    lane = grid_of(1)
    own = device * device
    alone = jnp.where(device == 0, 1, 0)
    for plane in range(6):
        half = plane % 2
        slot = 1 if plane // 2 == 1 else 0
        imaginary = plane // 2 == 2
        modes = row * row
        if half:
            modes = jnp.where(row == 0, square, modes)
        lane0 = lane == 0
        if slot:
            modes = modes + own + alone * square
            modes = modes + jnp.where(lane0, (1 - alone) * square, lane * lane)
        else:
            modes = modes + own + lane * lane
            pair = lane0 & (row == 0) if not half else (lane0 & (row != 0))
            if imaginary and half:
                pair = lane0
            if half or imaginary:
                modes = modes + jnp.where(pair, alone * (2 * square), 0)
        ksq = modes.astype(F32) * (wave_scale / N) ** 2
        lin = growth_rate - (1.0 - ksq) * (1.0 - ksq)
        scaled = time_step * lin
        (half_phi,) = phi_values(0.5 * scaled, (1,))
        first, second, third = phi_values(scaled, (1, 2, 3))
        factors[0, plane] = jnp.exp(0.5 * scaled)
        factors[1, plane] = 0.5 * time_step * half_phi
        factors[2, plane] = jnp.exp(scaled)
        factors[3, plane] = time_step * (first - 3.0 * second + 4.0 * third)
        factors[4, plane] = time_step * (second - 2.0 * third)
        factors[5, plane] = time_step * (4.0 * third - second)


def shape(*dims):
    return jax.ShapeDtypeStruct(dims, F32)


VMEM = pl.BlockSpec(memory_space=pltpu.VMEM)
HBM = pl.BlockSpec(memory_space=pltpu.HBM)


def call(kernel, outs, *args, name, ins=VMEM, into=VMEM, scratch=()):
    single = not isinstance(outs, tuple)
    return pl.pallas_call(
        kernel,
        out_shape=outs,
        in_specs=[ins] * len(args),
        out_specs=into if single else tuple(into for _ in outs),
        scratch_shapes=scratch,
        compiler_params=pltpu.CompilerParams(vmem_limit_bytes=16 << 20),
        name=name,
    )(*args)


def move(send):
    tiles = send.reshape(H, send.shape[0] // H, H)
    out = lax.all_to_all(tiles, BOTH, split_axis=0, concat_axis=0, tiled=True)
    return out.reshape(send.shape)


def body(tabs, field):
    message = shape(8 * H, H)
    spectrum = shape(8, H, H)
    send, factors, tabs = call(
        first_kernel,
        (shape(16 * H, H), shape(6, 6, H, H), jax.ShapeDtypeStruct(tabs.shape, BF16)),
        pltpu.with_memory_space_constraint(field, pltpu.HBM),
        pltpu.with_memory_space_constraint(tabs, pltpu.HBM),
        name="first",
        ins=HBM,
        scratch=[pltpu.VMEM(field.shape, F32), pltpu.SemaphoreType.DMA((7,))],
    )
    got = move(send)
    send, keep, base, total = call(
        spectral_first, (message, spectrum, spectrum, spectrum), got, factors, tabs, name="spectral_first"
    )

    def physical(send):
        return move(call(middle_kernel, message, move(send), tabs, name="physical"))

    for kept, twice in ((keep, False), (base, True)):
        got = physical(send)
        send, total = call(
            functools.partial(spectral_middle, twice=twice),
            (message, spectrum),
            got, factors, kept, total, tabs,
            name="spectral_middle",
        )
    got = physical(send)
    send = call(spectral_last, message, got, factors, total, tabs, name="spectral_last")
    return call(
        last_kernel,
        shape(*field.shape),
        move(send), tabs,
        name="last",
        into=HBM,
        scratch=[pltpu.VMEM(field.shape, F32), pltpu.SemaphoreType.DMA((2,))],
    )


def solution(mesh):
    tabs = np.stack([split_table(t) for t in tables()])
    placed = P(BOTH, None, None)

    def run(initial_field):
        return body(jnp.asarray(tabs), initial_field)

    return jax.shard_map(run, mesh=mesh, in_specs=(placed,), out_specs=placed, check_vma=False)
```

```python
import functools
import math

import jax
import jax.numpy as jnp
import numpy as np
from jax import lax
from jax.experimental import pallas as pl
from jax.experimental.pallas import tpu as pltpu
from jax.sharding import PartitionSpec as P

growth_rate = 0.3
quadratic = 1.0
time_step = 0.2
wave_scale = 4.0

N = 256
H = 128
BOTH = ("row", "col")
F32 = jnp.float32
BF16 = jnp.bfloat16


def tables():
    n = np.arange(N)
    j = np.arange(H)
    angle = 2.0 * np.pi / N * ((j[:, None] * n[None, :]) % N)
    cosine = np.cos(angle)
    sine = np.sin(angle)
    alternate = 1.0 - 2.0 * (n % 2)
    sine_alt = sine.copy()
    sine_alt[0] = alternate
    forward_y = np.concatenate([cosine, sine_alt])
    inverse_y = forward_y.T / N
    order = np.concatenate([np.arange(0, N, 2), np.arange(1, N, 2)])
    forward_x = forward_y[:, order]
    inverse_x = inverse_y[order]
    minus = -sine
    minus[0] = alternate
    forward_z = np.concatenate([cosine, minus]).T
    weight = np.where(j == 0, 1.0, 2.0)[:, None] / N
    inverse_z = np.concatenate([cosine * weight, minus * weight])
    return forward_z, forward_y, forward_x, inverse_x, inverse_y, inverse_z


FZ, FY, FX, IX, IY, IZ = range(6)


def split_table(table):
    high = np.asarray(table, np.float32).astype(jnp.bfloat16)
    low = (table - high.astype(np.float64)).astype(np.float32).astype(jnp.bfloat16)
    return np.stack([high, low])


def split(values):
    high = values.astype(BF16)
    low = (values - high.astype(F32)).astype(BF16)
    return high, low


def dot(left, right):
    return jnp.dot(left, right, preferred_element_type=F32)


def table_left(table, parts, at=0, count=N):
    high, low = parts
    top, bottom = table[0, pl.ds(at, count), :], table[1, pl.ds(at, count), :]
    return dot(top, high) + (dot(top, low) + dot(bottom, high))


def table_right(values, table):
    high, low = split(values)
    return dot(high, table[0]) + (dot(low, table[0]) + dot(high, table[1]))


def grid_of(axis):
    return lax.broadcasted_iota(jnp.int32, (H, H), axis)


def quarters(whole):
    return whole[:H, :H], whole[:H, H:], whole[H:, :H], whole[H:, H:]


def joined(top_left, top_right, bottom_left, bottom_right):
    return jnp.concatenate(
        [
            jnp.concatenate([top_left, top_right], axis=1),
            jnp.concatenate([bottom_left, bottom_right], axis=1),
        ],
        axis=0,
    )


def tile_rows(ref, slot):
    return ref[pl.ds(slot, H, stride=ref.shape[0] // H), :]


def put_rows(ref, slot, values):
    ref[pl.ds(slot, H, stride=ref.shape[0] // H), :] = values


def reaction(values):
    return quadratic * values * values - values * values * values


def send_modes(whole, send, base):
    cre, cim, sre, sim = quarters(whole)
    lane0 = grid_of(1) == 0
    row0 = grid_of(0) == 0
    corner = lane0 & row0
    o0re = jnp.where(lane0 | row0, cre, cre + sim)
    o0im = jnp.where(lane0, -sre, cim - sre)
    o0im = jnp.where(row0, cim, o0im)
    o0im = jnp.where(corner, sim, o0im)
    o1re = jnp.where(row0, sre, cre - sim)
    o1re = jnp.where(lane0, cim, o1re)
    o1im = jnp.where(lane0, -sim, cim + sre)
    o1im = jnp.where(row0, sim, o1im)
    o1im = jnp.where(corner, sre, o1im)
    put_rows(send, base + 0, o0re)
    put_rows(send, base + 1, o0im)
    put_rows(send, base + 2, o1re)
    put_rows(send, base + 3, o1im)


def got_modes(got, base):
    s0re = tile_rows(got, base + 0)
    s0im = tile_rows(got, base + 1)
    s1re = tile_rows(got, base + 2)
    s1im = tile_rows(got, base + 3)
    lane0 = grid_of(1) == 0
    row0 = grid_of(0) == 0
    corner = lane0 & row0
    pre = jnp.where(lane0, 2.0 * s0re, s0re + s1re)
    pre = jnp.where(row0, s0re, pre)
    pim = jnp.where(lane0, 2.0 * s1re, s0im + s1im)
    pim = jnp.where(row0, s0im, pim)
    pim = jnp.where(corner, s1re, pim)
    mre = jnp.where(lane0, -2.0 * s0im, s1im - s0im)
    mre = jnp.where(row0, s1re, mre)
    mre = jnp.where(corner, s1im, mre)
    mim = jnp.where(lane0, -2.0 * s1im, s0re - s1re)
    mim = jnp.where(row0, s1im, mim)
    mim = jnp.where(corner, s0im, mim)
    return joined(pre, pim, mre, mim)


ROWS = range(2)
HALVES = range(2)
PIECES = [(row, half) for row in ROWS for half in HALVES]


def from_messages(got, iy, iz):
    modes = [split(got_modes(got, 4 * row)) for row in ROWS]
    parts = [table_left(iy, modes[row], H * half, H) for row, half in PIECES]
    return [table_right(part, iz) for part in parts]


def to_messages(fields, send, fz, fy):
    parts = [[table_right(piece, fz) for piece in field] for field in fields]
    whole = [
        split(jnp.concatenate(part[2 * row : 2 * row + 2], axis=0)) for part in parts for row in ROWS
    ]
    for slot, modes in enumerate(whole):
        send_modes(table_left(fy, modes), send, 4 * slot)


def first_kernel(field_hbm, tabs_hbm, send, factors, tabs, field, sems):
    def load(source, target, at):
        return pltpu.make_async_copy(source, target, sems.at[at])

    own = load(field_hbm, field, 0)
    loads = [load(tabs_hbm.at[k], tabs.at[k], 1 + k) for k in range(6)]
    own.start()
    for one in loads:
        one.start()
    factor_kernel(factors)
    own.wait()
    loads[FZ].wait()
    loads[FY].wait()
    pieces = [field[row, pl.ds(H * half, H), :] for row, half in PIECES]
    to_messages([pieces, [reaction(v) for v in pieces]], send, tabs.at[FZ], tabs.at[FY])
    for k in (FX, IX, IY, IZ):
        loads[k].wait()


def middle_kernel(got, tabs, send):
    pieces = from_messages(got, tabs.at[IY], tabs.at[IZ])
    to_messages([[reaction(v) for v in pieces]], send, tabs.at[FZ], tabs.at[FY])


def last_kernel(got, tabs, field_hbm, field, sems):
    stores = []
    pieces = from_messages(got, tabs.at[IY], tabs.at[IZ])
    for k, (row, half) in enumerate(PIECES):
        at = pl.ds(H * half, H)
        field[row, at, :] = pieces[k]
        one = pltpu.make_async_copy(field.at[row, at], field_hbm.at[row, at], sems.at[k])
        one.start()
        stores.append(one)
    for one in stores:
        one.wait()


def special_lane(slot):
    if slot:
        return None
    device = lax.axis_index(BOTH)
    lane = grid_of(1) + jnp.where(device == 0, 0, H)
    return (lane == 0) & (grid_of(0) != 0)


def column_of(got, slot, field=0):
    at = 8 * field + 2 * slot
    column = joined(*(tile_rows(got, at + k) for k in (0, 1, 4, 5)))
    return split(column)


def modes_of(whole, slot):
    cre, cim, sre, sim = quarters(whole)
    row0 = grid_of(0) == 0
    tre = jnp.where(row0, cre, cre + sim)
    tim = jnp.where(row0, cim, cim - sre)
    bre = jnp.where(row0, sre, cre - sim)
    bim = jnp.where(row0, sim, cim + sre)
    special = special_lane(slot)
    if special is not None:
        tre = jnp.where(special, cre, tre)
        tim = jnp.where(special, -sre, tim)
        bre = jnp.where(special, cim, bre)
        bim = jnp.where(special, -sim, bim)
    return tre, tim, bre, bim


def spectra_of(got, fx, fields=1):
    keys = [(slot, field) for slot in range(2) for field in range(fields)]
    columns = [column_of(got, *key) for key in keys]
    wholes = [table_left(fx, column) for column in columns]
    return {key: modes_of(whole, key[0]) for key, whole in zip(keys, wholes)}


def operand_of(parts, slot):
    tre, tim, bre, bim = parts
    row0 = grid_of(0) == 0
    pre = jnp.where(row0, tre, tre + bre)
    pim = jnp.where(row0, tim, tim + bim)
    mre = jnp.where(row0, bre, bim - tim)
    mim = jnp.where(row0, bim, tre - bre)
    special = special_lane(slot)
    if special is not None:
        pre = jnp.where(special, 2.0 * tre, pre)
        pim = jnp.where(special, 2.0 * bre, pim)
        mre = jnp.where(special, -2.0 * tim, mre)
        mim = jnp.where(special, -2.0 * bim, mim)
    return split(joined(pre, pim, mre, mim))


def spectra_to(nexts, ix, send):
    operands = [operand_of(parts, slot) for slot, parts in enumerate(nexts)]
    for slot, operand in enumerate(operands):
        for row in ROWS:
            out = table_left(ix, operand, H * row, H)
            put_rows(send, 4 * row + 2 * slot, out[:, :H])
            put_rows(send, 4 * row + 2 * slot + 1, out[:, H:])


def plane_of(slot, half, part):
    if slot:
        return 2 + half
    return (4 if part else 0) + half


def each_part():
    for half in range(2):
        for part in range(2):
            yield 2 * half + part, half, part


def spectral_first(got, factors, tabs, send, keep, base, total):
    spectra = spectra_of(got, tabs.at[FX], 2)
    nexts = [[], []]
    for slot in range(2):
        state, react = spectra[slot, 0], spectra[slot, 1]
        for k, half, part in each_part():
            plane = plane_of(slot, half, part)
            e_half = factors[0, plane]
            q_half = factors[1, plane]
            kept = e_half * state[k]
            turn = q_half * react[k]
            first = kept + turn
            keep[4 * slot + k] = kept
            base[4 * slot + k] = e_half * first - turn
            total[4 * slot + k] = factors[2, plane] * state[k] + factors[3, plane] * react[k]
            nexts[slot].append(first)
    spectra_to(nexts, tabs.at[IX], send)


def spectral_middle(got, factors, kept, total, tabs, send, total_out, *, twice):
    spectra = spectra_of(got, tabs.at[FX])
    nexts = [[], []]
    for slot in range(2):
        react = spectra[slot, 0]
        for k, half, part in each_part():
            plane = plane_of(slot, half, part)
            turn = factors[1, plane] * react[k]
            if twice:
                turn = 2.0 * turn
            nexts[slot].append(kept[4 * slot + k] + turn)
            total_out[4 * slot + k] = total[4 * slot + k] + 2.0 * factors[4, plane] * react[k]
    spectra_to(nexts, tabs.at[IX], send)


def spectral_last(got, factors, total, tabs, send):
    spectra = spectra_of(got, tabs.at[FX])
    nexts = [[], []]
    for slot in range(2):
        react = spectra[slot, 0]
        for k, half, part in each_part():
            plane = plane_of(slot, half, part)
            nexts[slot].append(total[4 * slot + k] + factors[5, plane] * react[k])
    spectra_to(nexts, tabs.at[IX], send)


def phi_values(argument, degrees):
    within = jnp.abs(argument) < 1.0
    inside = jnp.where(within, argument, 0.0)
    outside = jnp.where(within, 2.0, argument)
    series = []
    for degree in degrees:
        running = jnp.zeros_like(argument) + 1.0 / math.factorial(11 + degree)
        for exponent in range(10, -1, -1):
            running = running * inside + 1.0 / math.factorial(exponent + degree)
        series.append(running)
    growth = jnp.exp(outside)
    closed = [(growth - 1.0) / outside]
    if len(degrees) > 1:
        square = outside * outside
        closed.append((growth - 1.0 - outside) / square)
        closed.append((growth - 1.0 - outside - 0.5 * square) / (square * outside))
    return [jnp.where(within, s, c) for s, c in zip(series, closed)]


def factor_kernel(factors):
    device = lax.axis_index(BOTH)
    square = H * H
    row = grid_of(0)
    lane = grid_of(1)
    own = device * device
    alone = jnp.where(device == 0, 1, 0)
    for plane in range(6):
        half = plane % 2
        slot = 1 if plane // 2 == 1 else 0
        imaginary = plane // 2 == 2
        modes = row * row
        if half:
            modes = jnp.where(row == 0, square, modes)
        lane0 = lane == 0
        if slot:
            modes = modes + own + alone * square
            modes = modes + jnp.where(lane0, (1 - alone) * square, lane * lane)
        else:
            modes = modes + own + lane * lane
            pair = lane0 & (row == 0) if not half else (lane0 & (row != 0))
            if imaginary and half:
                pair = lane0
            if half or imaginary:
                modes = modes + jnp.where(pair, alone * (2 * square), 0)
        ksq = modes.astype(F32) * (wave_scale / N) ** 2
        lin = growth_rate - (1.0 - ksq) * (1.0 - ksq)
        scaled = time_step * lin
        (half_phi,) = phi_values(0.5 * scaled, (1,))
        first, second, third = phi_values(scaled, (1, 2, 3))
        factors[0, plane] = jnp.exp(0.5 * scaled)
        factors[1, plane] = 0.5 * time_step * half_phi
        factors[2, plane] = jnp.exp(scaled)
        factors[3, plane] = time_step * (first - 3.0 * second + 4.0 * third)
        factors[4, plane] = time_step * (second - 2.0 * third)
        factors[5, plane] = time_step * (4.0 * third - second)


def shape(*dims):
    return jax.ShapeDtypeStruct(dims, F32)


VMEM = pl.BlockSpec(memory_space=pltpu.VMEM)
HBM = pl.BlockSpec(memory_space=pltpu.HBM)


def call(kernel, outs, *args, name, ins=VMEM, into=VMEM, scratch=()):
    single = not isinstance(outs, tuple)
    return pl.pallas_call(
        kernel,
        out_shape=outs,
        in_specs=[ins] * len(args),
        out_specs=into if single else tuple(into for _ in outs),
        scratch_shapes=scratch,
        compiler_params=pltpu.CompilerParams(vmem_limit_bytes=16 << 20),
        name=name,
    )(*args)


def move(send):
    tiles = send.reshape(H, send.shape[0] // H, H)
    out = lax.all_to_all(tiles, BOTH, split_axis=0, concat_axis=0, tiled=True)
    return out.reshape(send.shape)


def body(tabs, field):
    message = shape(8 * H, H)
    spectrum = shape(8, H, H)
    send, factors, tabs = call(
        first_kernel,
        (shape(16 * H, H), shape(6, 6, H, H), jax.ShapeDtypeStruct(tabs.shape, BF16)),
        pltpu.with_memory_space_constraint(field, pltpu.HBM),
        pltpu.with_memory_space_constraint(tabs, pltpu.HBM),
        name="first",
        ins=HBM,
        scratch=[pltpu.VMEM(field.shape, F32), pltpu.SemaphoreType.DMA((7,))],
    )
    got = move(send)
    send, keep, base, total = call(
        spectral_first, (message, spectrum, spectrum, spectrum), got, factors, tabs, name="spectral_first"
    )

    def physical(send):
        return move(call(middle_kernel, message, move(send), tabs, name="physical"))

    for kept, twice in ((keep, False), (base, True)):
        got = physical(send)
        send, total = call(
            functools.partial(spectral_middle, twice=twice),
            (message, spectrum),
            got, factors, kept, total, tabs,
            name="spectral_middle",
        )
    got = physical(send)
    send = call(spectral_last, message, got, factors, total, tabs, name="spectral_last")
    return call(
        last_kernel,
        shape(*field.shape),
        move(send), tabs,
        name="last",
        into=HBM,
        scratch=[pltpu.VMEM(field.shape, F32), pltpu.SemaphoreType.DMA((4,))],
    )


def solution(mesh):
    tabs = np.stack([split_table(t) for t in tables()])
    placed = P(BOTH, None, None)

    def run(initial_field):
        return body(jnp.asarray(tabs), initial_field)

    return jax.shard_map(run, mesh=mesh, in_specs=(placed,), out_specs=placed, check_vma=False)
```

```python
import functools
import math

import jax
import jax.numpy as jnp
import numpy as np
from jax import lax
from jax.experimental import pallas as pl
from jax.experimental.pallas import tpu as pltpu
from jax.sharding import PartitionSpec as P

growth_rate = 0.3
quadratic = 1.0
time_step = 0.2
wave_scale = 4.0

N = 256
H = 128
Q = 64
BOTH = ("row", "col")
F32 = jnp.float32
BF16 = jnp.bfloat16


def tables():
    n = np.arange(N)
    j = np.arange(H)
    angle = 2.0 * np.pi / N * ((j[:, None] * n[None, :]) % N)
    cosine = np.cos(angle)
    sine = np.sin(angle)
    alternate = 1.0 - 2.0 * (n % 2)
    sine_alt = sine.copy()
    sine_alt[0] = alternate
    forward_y = np.concatenate([cosine, sine_alt])
    inverse_y = forward_y.T / N
    order = np.concatenate([np.arange(0, N, 2), np.arange(1, N, 2)])
    pieces = np.arange(N).reshape(2, 2, Q).transpose(1, 0, 2).reshape(N)
    inverse_x = inverse_y[order]
    forward_y = forward_y[pieces]
    forward_x = forward_y[:, order]
    minus = -sine
    minus[0] = alternate
    forward_z = np.concatenate([cosine, minus]).T
    weight = np.where(j == 0, 1.0, 2.0)[:, None] / N
    inverse_z = np.concatenate([cosine * weight, minus * weight])
    return forward_z, forward_y, forward_x, inverse_x, inverse_y, inverse_z


FZ, FY, FX, IX, IY, IZ = range(6)


def split_table(table):
    high = np.asarray(table, np.float32).astype(jnp.bfloat16)
    low = (table - high.astype(np.float64)).astype(np.float32).astype(jnp.bfloat16)
    return np.stack([high, low])


def split(values):
    high = values.astype(BF16)
    low = (values - high.astype(F32)).astype(BF16)
    return high, low


def dot(left, right):
    return jnp.dot(left, right, preferred_element_type=F32)


def table_left(table, parts, at=0, count=N):
    high, low = parts
    top, bottom = table[0, pl.ds(at, count), :], table[1, pl.ds(at, count), :]
    return dot(top, high) + (dot(top, low) + dot(bottom, high))


def table_right(values, table):
    high, low = split(values)
    return dot(high, table[0]) + (dot(low, table[0]) + dot(high, table[1]))


def grid_of(axis):
    return lax.broadcasted_iota(jnp.int32, (H, H), axis)


def piece_grid(axis):
    return lax.broadcasted_iota(jnp.int32, (Q, H), axis)


def first_row(piece):
    return None if piece else piece_grid(0) == 0


def pick(mask, chosen, other):
    return other if mask is None else jnp.where(mask, chosen, other)


def quarters(whole):
    return whole[:Q, :H], whole[:Q, H:], whole[Q:, :H], whole[Q:, H:]


def joined(top_left, top_right, bottom_left, bottom_right):
    return jnp.concatenate(
        [
            jnp.concatenate([top_left, top_right], axis=1),
            jnp.concatenate([bottom_left, bottom_right], axis=1),
        ],
        axis=0,
    )


def tile_rows(ref, slot):
    return ref[pl.ds(slot, H, stride=ref.shape[0] // H), :]


def put_rows(ref, slot, values, at=0):
    stride = ref.shape[0] // H
    ref[pl.ds(slot + stride * at, values.shape[0], stride=stride), :] = values


def reaction(values):
    return quadratic * values * values - values * values * values


def send_modes(whole, piece, send, base):
    cre, cim, sre, sim = quarters(whole)
    lane0 = piece_grid(1) == 0
    row0 = first_row(piece)
    corner = None if row0 is None else lane0 & row0
    o0re = jnp.where(lane0 if row0 is None else lane0 | row0, cre, cre + sim)
    o0im = pick(row0, cim, jnp.where(lane0, -sre, cim - sre))
    o0im = pick(corner, sim, o0im)
    o1re = jnp.where(lane0, cim, pick(row0, sre, cre - sim))
    o1im = pick(row0, sim, jnp.where(lane0, -sim, cim + sre))
    o1im = pick(corner, sre, o1im)
    for k, values in enumerate((o0re, o0im, o1re, o1im)):
        put_rows(send, base + k, values, Q * piece)


def got_modes(got, base):
    s0re = tile_rows(got, base + 0)
    s0im = tile_rows(got, base + 1)
    s1re = tile_rows(got, base + 2)
    s1im = tile_rows(got, base + 3)
    lane0 = grid_of(1) == 0
    row0 = grid_of(0) == 0
    corner = lane0 & row0
    pre = jnp.where(lane0, 2.0 * s0re, s0re + s1re)
    pre = jnp.where(row0, s0re, pre)
    pim = jnp.where(lane0, 2.0 * s1re, s0im + s1im)
    pim = jnp.where(row0, s0im, pim)
    pim = jnp.where(corner, s1re, pim)
    mre = jnp.where(lane0, -2.0 * s0im, s1im - s0im)
    mre = jnp.where(row0, s1re, mre)
    mre = jnp.where(corner, s1im, mre)
    mim = jnp.where(lane0, -2.0 * s1im, s0re - s1re)
    mim = jnp.where(row0, s1im, mim)
    mim = jnp.where(corner, s0im, mim)
    return joined(pre, pim, mre, mim)


ROWS = range(2)
HALVES = range(2)
PIECES = [(row, half) for row in ROWS for half in HALVES]


def from_messages(got, iy, iz):
    modes = [split(got_modes(got, 4 * row)) for row in ROWS]
    parts = [table_left(iy, modes[row], H * half, H) for row, half in PIECES]
    return [table_right(part, iz) for part in parts]


def to_messages(fields, send, fz, fy):
    parts = [[table_right(piece, fz) for piece in field] for field in fields]
    whole = [
        split(jnp.concatenate(part[2 * row : 2 * row + 2], axis=0)) for part in parts for row in ROWS
    ]
    for slot, modes in enumerate(whole):
        for piece in range(2):
            send_modes(table_left(fy, modes, H * piece, H), piece, send, 4 * slot)


def first_kernel(field_hbm, tabs_hbm, send, factors, tabs, field, sems):
    def load(source, target, at):
        return pltpu.make_async_copy(source, target, sems.at[at])

    own = load(field_hbm, field, 0)
    loads = [load(tabs_hbm.at[k], tabs.at[k], 1 + k) for k in range(6)]
    for one in (own, loads[FZ], loads[FY]):
        one.start()
    factor_kernel(factors)
    for one in (own, loads[FZ], loads[FY]):
        one.wait()
    for k in (FX, IX, IY, IZ):
        loads[k].start()
    pieces = [field[row, pl.ds(H * half, H), :] for row, half in PIECES]
    to_messages([pieces, [reaction(v) for v in pieces]], send, tabs.at[FZ], tabs.at[FY])
    for k in (FX, IX, IY, IZ):
        loads[k].wait()


def middle_kernel(got, tabs, send):
    pieces = from_messages(got, tabs.at[IY], tabs.at[IZ])
    to_messages([[reaction(v) for v in pieces]], send, tabs.at[FZ], tabs.at[FY])


def last_kernel(got, tabs, field_hbm, field, sems):
    stores = []
    pieces = from_messages(got, tabs.at[IY], tabs.at[IZ])
    for k, (row, half) in enumerate(PIECES):
        at = pl.ds(H * half, H)
        field[row, at, :] = pieces[k]
        one = pltpu.make_async_copy(field.at[row, at], field_hbm.at[row, at], sems.at[k])
        one.start()
        stores.append(one)
    for one in stores:
        one.wait()


def special_lane(slot, row0):
    if slot:
        return None
    device = lax.axis_index(BOTH)
    lane = piece_grid(1) + jnp.where(device == 0, 0, H) == 0
    return lane if row0 is None else lane & ~row0


def column_of(got, slot, field=0):
    at = 8 * field + 2 * slot
    column = joined(*(tile_rows(got, at + k) for k in (0, 1, 4, 5)))
    return split(column)


def modes_of(whole, slot, piece):
    cre, cim, sre, sim = quarters(whole)
    row0 = first_row(piece)
    special = special_lane(slot, row0)
    tre = pick(special, cre, pick(row0, cre, cre + sim))
    tim = pick(special, -sre, pick(row0, cim, cim - sre))
    bre = pick(special, cim, pick(row0, sre, cre - sim))
    bim = pick(special, -sim, pick(row0, sim, cim + sre))
    return tre, tim, bre, bim


PARTS = [(slot, piece) for slot in range(2) for piece in range(2)]


def spectra_of(got, fx, fields=1):
    keys = [(slot, field) for slot in range(2) for field in range(fields)]
    columns = {key: column_of(got, *key) for key in keys}
    return {
        (slot, piece): [
            modes_of(table_left(fx, columns[slot, field], H * piece, H), slot, piece)
            for field in range(fields)
        ]
        for slot, piece in PARTS
    }


def operand_of(parts, slot, piece):
    tre, tim, bre, bim = parts
    row0 = first_row(piece)
    special = special_lane(slot, row0)
    pre = pick(special, 2.0 * tre, pick(row0, tre, tre + bre))
    pim = pick(special, 2.0 * bre, pick(row0, tim, tim + bim))
    mre = pick(special, -2.0 * tim, pick(row0, bre, bim - tim))
    mim = pick(special, -2.0 * bim, pick(row0, bim, tre - bre))
    plus = split(jnp.concatenate([pre, pim], axis=1))
    minus = split(jnp.concatenate([mre, mim], axis=1))
    return plus, minus


def spectra_to(nexts, ix, send):
    sides = {key: operand_of(nexts[key], *key) for key in PARTS}
    for slot in range(2):
        one, two = sides[slot, 0], sides[slot, 1]
        operand = [
            jnp.concatenate([one[0][k], two[0][k], one[1][k], two[1][k]], axis=0) for k in range(2)
        ]
        for row in ROWS:
            out = table_left(ix, operand, H * row, H)
            put_rows(send, 4 * row + 2 * slot, out[:, :H])
            put_rows(send, 4 * row + 2 * slot + 1, out[:, H:])


def plane_of(slot, half, part):
    if slot:
        return 2 + half
    return (4 if part else 0) + half


def each_part(slot, piece):
    rows = pl.ds(Q * piece, Q)
    for half in range(2):
        for part in range(2):
            k = 2 * half + part
            yield k, (4 * slot + k, rows), (plane_of(slot, half, part), rows)


def spectral_first(got, factors, tabs, send, keep, base, total):
    spectra = spectra_of(got, tabs.at[FX], 2)
    nexts = {}
    for key in PARTS:
        state, react = spectra[key]
        nexts[key] = []
        for k, own, plane in each_part(*key):
            e_half = factors[0, *plane]
            q_half = factors[1, *plane]
            kept = e_half * state[k]
            turn = q_half * react[k]
            first = kept + turn
            keep[own] = kept
            base[own] = e_half * first - turn
            total[own] = factors[2, *plane] * state[k] + factors[3, *plane] * react[k]
            nexts[key].append(first)
    spectra_to(nexts, tabs.at[IX], send)


def spectral_middle(got, factors, kept, total, tabs, send, total_out, *, twice):
    spectra = spectra_of(got, tabs.at[FX])
    nexts = {}
    for key in PARTS:
        (react,) = spectra[key]
        nexts[key] = []
        for k, own, plane in each_part(*key):
            turn = factors[1, *plane] * react[k]
            if twice:
                turn = 2.0 * turn
            nexts[key].append(kept[own] + turn)
            total_out[own] = total[own] + 2.0 * factors[4, *plane] * react[k]
    spectra_to(nexts, tabs.at[IX], send)


def spectral_last(got, factors, total, tabs, send):
    spectra = spectra_of(got, tabs.at[FX])
    nexts = {}
    for key in PARTS:
        (react,) = spectra[key]
        nexts[key] = [
            total[own] + factors[5, *plane] * react[k] for k, own, plane in each_part(*key)
        ]
    spectra_to(nexts, tabs.at[IX], send)


def step_factors(ksq):
    lin = growth_rate - (1.0 - ksq) * (1.0 - ksq)
    z = time_step * lin
    e_half = jnp.exp(0.5 * z)
    e_full = e_half * e_half
    within = jnp.abs(z) < 1.0
    inside = jnp.where(within, z, 0.0)
    inverse = 1.0 / jnp.where(within, 2.0, z)
    series = jnp.full_like(z, 1.0 / math.factorial(14))
    for exponent in range(10, -1, -1):
        series = series * inside + 1.0 / math.factorial(exponent + 3)
    closed_one = (e_full - 1.0) * inverse
    closed_two = (closed_one - 1.0) * inverse
    third = jnp.where(within, series, (closed_two - 0.5) * inverse)
    second = jnp.where(within, 0.5 + inside * series, closed_two)
    first = jnp.where(within, 1.0 + inside * second, closed_one)
    return (
        e_half,
        time_step * first / (e_half + 1.0),
        e_full,
        time_step * (first - 3.0 * second + 4.0 * third),
        time_step * (second - 2.0 * third),
        time_step * (4.0 * third - second),
    )


def factor_kernel(factors):
    device = lax.axis_index(BOTH)
    square = H * H
    own = device * device
    alone = jnp.where(device == 0, 1, 0)

    def fill(plane, count):
        row = lax.broadcasted_iota(jnp.int32, (count, H), 0)
        lane = lax.broadcasted_iota(jnp.int32, (count, H), 1)
        half, kind = plane % 2, plane // 2
        lane0 = lane == 0
        modes = row * row
        if half:
            modes = jnp.where(row == 0, square, modes)
        if kind == 1:
            modes = modes + own + alone * square
            modes = modes + jnp.where(lane0, (1 - alone) * square, lane * lane)
        else:
            modes = modes + own + lane * lane
            pair = lane0 & (row != 0)
            if kind == 2:
                pair = lane0 if half else lane0 & (row == 0)
            if half or kind == 2:
                modes = modes + jnp.where(pair, alone * (2 * square), 0)
        values = step_factors(modes.astype(F32) * (wave_scale / N) ** 2)
        for k in range(6):
            factors[k, plane, pl.ds(0, count), :] = values[k]
            if kind == 0:
                factors[k, plane + 4, pl.ds(8, H - 8), :] = values[k][8:]

    for plane in range(4):
        fill(plane, H)
    for plane in (4, 5):
        fill(plane, 8)


def shape(*dims):
    return jax.ShapeDtypeStruct(dims, F32)


VMEM = pl.BlockSpec(memory_space=pltpu.VMEM)
HBM = pl.BlockSpec(memory_space=pltpu.HBM)


def call(kernel, outs, *args, name, ins=VMEM, into=VMEM, scratch=()):
    single = not isinstance(outs, tuple)
    return pl.pallas_call(
        kernel,
        out_shape=outs,
        in_specs=[ins] * len(args),
        out_specs=into if single else tuple(into for _ in outs),
        scratch_shapes=scratch,
        compiler_params=pltpu.CompilerParams(vmem_limit_bytes=16 << 20),
        name=name,
    )(*args)


def move(send):
    tiles = send.reshape(H, send.shape[0] // H, H)
    out = lax.all_to_all(tiles, BOTH, split_axis=0, concat_axis=0, tiled=True)
    return out.reshape(send.shape)


def body(tabs, field):
    message = shape(8 * H, H)
    spectrum = shape(8, H, H)
    send, factors, tabs = call(
        first_kernel,
        (shape(16 * H, H), shape(6, 6, H, H), jax.ShapeDtypeStruct(tabs.shape, BF16)),
        pltpu.with_memory_space_constraint(field, pltpu.HBM),
        pltpu.with_memory_space_constraint(tabs, pltpu.HBM),
        name="first",
        ins=HBM,
        scratch=[pltpu.VMEM(field.shape, F32), pltpu.SemaphoreType.DMA((7,))],
    )
    got = move(send)
    send, keep, base, total = call(
        spectral_first, (message, spectrum, spectrum, spectrum), got, factors, tabs, name="spectral_first"
    )

    def physical(send):
        return move(call(middle_kernel, message, move(send), tabs, name="physical"))

    for kept, twice in ((keep, False), (base, True)):
        got = physical(send)
        send, total = call(
            functools.partial(spectral_middle, twice=twice),
            (message, spectrum),
            got, factors, kept, total, tabs,
            name="spectral_middle",
        )
    got = physical(send)
    send = call(spectral_last, message, got, factors, total, tabs, name="spectral_last")
    return call(
        last_kernel,
        shape(*field.shape),
        move(send), tabs,
        name="last",
        into=HBM,
        scratch=[pltpu.VMEM(field.shape, F32), pltpu.SemaphoreType.DMA((4,))],
    )


def solution(mesh):
    tabs = np.stack([split_table(t) for t in tables()])
    placed = P(BOTH, None, None)

    def run(initial_field):
        return body(jnp.asarray(tabs), initial_field)

    return jax.shard_map(run, mesh=mesh, in_specs=(placed,), out_specs=placed, check_vma=False)
```

```python
import functools
import math

import jax
import jax.numpy as jnp
import numpy as np
from jax import lax
from jax.experimental import pallas as pl
from jax.experimental.pallas import tpu as pltpu
from jax.sharding import PartitionSpec as P

growth_rate = 0.3
quadratic = 1.0
time_step = 0.2
wave_scale = 4.0

N = 256
H = 128
Q = 64
BOTH = ("row", "col")
F32 = jnp.float32
BF16 = jnp.bfloat16


def tables():
    n = np.arange(N)
    j = np.arange(H)
    angle = 2.0 * np.pi / N * ((j[:, None] * n[None, :]) % N)
    cosine = np.cos(angle)
    sine = np.sin(angle)
    alternate = 1.0 - 2.0 * (n % 2)
    sine_alt = sine.copy()
    sine_alt[0] = alternate
    forward_y = np.concatenate([cosine, sine_alt])
    inverse_y = forward_y.T / N
    order = np.concatenate([np.arange(0, N, 2), np.arange(1, N, 2)])
    pieces = np.arange(N).reshape(2, 2, Q).transpose(1, 0, 2).reshape(N)
    inverse_x = inverse_y[order]
    forward_y = forward_y[pieces]
    forward_x = forward_y[:, order]
    minus = -sine
    minus[0] = alternate
    forward_z = np.concatenate([cosine, minus]).T
    weight = np.where(j == 0, 1.0, 2.0)[:, None] / N
    inverse_z = np.concatenate([cosine * weight, minus * weight])
    return forward_z, forward_y, forward_x, inverse_x, inverse_y, inverse_z


FZ, FY, FX, IX, IY, IZ = range(6)


def split_table(table):
    high = np.asarray(table, np.float32).astype(jnp.bfloat16)
    low = (table - high.astype(np.float64)).astype(np.float32).astype(jnp.bfloat16)
    return np.stack([high, low])


def split(values):
    high = values.astype(BF16)
    low = (values - high.astype(F32)).astype(BF16)
    return high, low


def dot(left, right):
    return jnp.dot(left, right, preferred_element_type=F32)


def folded(whole):
    count = whole.shape[0] // 2
    return whole[:count], whole[count:]


def table_left(table, parts, at=0, count=N):
    high, low = parts
    top, bottom = table[0, pl.ds(at, count), :], table[1, pl.ds(at, count), :]
    main, rest = folded(dot(jnp.concatenate([top, bottom], axis=0), high))
    return main + (rest + dot(top, low))


def table_right(values, table):
    high, low = split(values)
    main, rest = folded(dot(jnp.concatenate([high, low], axis=0), table[0]))
    return main + (rest + dot(high, table[1]))


def grid_of(axis):
    return lax.broadcasted_iota(jnp.int32, (H, H), axis)


def piece_grid(axis):
    return lax.broadcasted_iota(jnp.int32, (Q, H), axis)


def first_row(piece):
    return None if piece else piece_grid(0) == 0


def pick(mask, chosen, other):
    return other if mask is None else jnp.where(mask, chosen, other)


def quarters(whole):
    return whole[:Q, :H], whole[:Q, H:], whole[Q:, :H], whole[Q:, H:]


def joined(top_left, top_right, bottom_left, bottom_right):
    return jnp.concatenate(
        [
            jnp.concatenate([top_left, top_right], axis=1),
            jnp.concatenate([bottom_left, bottom_right], axis=1),
        ],
        axis=0,
    )


def tile_rows(ref, slot):
    return ref[pl.ds(slot, H, stride=ref.shape[0] // H), :]


def put_rows(ref, slot, values, at=0):
    stride = ref.shape[0] // H
    ref[pl.ds(slot + stride * at, values.shape[0], stride=stride), :] = values


def reaction(values):
    return quadratic * values * values - values * values * values


def send_modes(whole, piece, send, base):
    cre, cim, sre, sim = quarters(whole)
    lane0 = piece_grid(1) == 0
    row0 = first_row(piece)
    corner = None if row0 is None else lane0 & row0
    o0re = jnp.where(lane0 if row0 is None else lane0 | row0, cre, cre + sim)
    o0im = pick(row0, cim, jnp.where(lane0, -sre, cim - sre))
    o0im = pick(corner, sim, o0im)
    o1re = jnp.where(lane0, cim, pick(row0, sre, cre - sim))
    o1im = pick(row0, sim, jnp.where(lane0, -sim, cim + sre))
    o1im = pick(corner, sre, o1im)
    for k, values in enumerate((o0re, o0im, o1re, o1im)):
        put_rows(send, base + k, values, Q * piece)


def got_modes(got, base):
    s0re = tile_rows(got, base + 0)
    s0im = tile_rows(got, base + 1)
    s1re = tile_rows(got, base + 2)
    s1im = tile_rows(got, base + 3)
    lane0 = grid_of(1) == 0
    row0 = grid_of(0) == 0
    corner = lane0 & row0
    pre = jnp.where(lane0, 2.0 * s0re, s0re + s1re)
    pre = jnp.where(row0, s0re, pre)
    pim = jnp.where(lane0, 2.0 * s1re, s0im + s1im)
    pim = jnp.where(row0, s0im, pim)
    pim = jnp.where(corner, s1re, pim)
    mre = jnp.where(lane0, -2.0 * s0im, s1im - s0im)
    mre = jnp.where(row0, s1re, mre)
    mre = jnp.where(corner, s1im, mre)
    mim = jnp.where(lane0, -2.0 * s1im, s0re - s1re)
    mim = jnp.where(row0, s1im, mim)
    mim = jnp.where(corner, s0im, mim)
    return joined(pre, pim, mre, mim)


ROWS = range(2)
HALVES = range(2)
PIECES = [(row, half) for row in ROWS for half in HALVES]


def from_messages(got, iy, iz):
    modes = [split(got_modes(got, 4 * row)) for row in ROWS]
    parts = [table_left(iy, modes[row], H * half, H) for row, half in PIECES]
    return [table_right(part, iz) for part in parts]


def to_messages(fields, send, fz, fy):
    parts = [[table_right(piece, fz) for piece in field] for field in fields]
    whole = [
        split(jnp.concatenate(part[2 * row : 2 * row + 2], axis=0)) for part in parts for row in ROWS
    ]
    for slot, modes in enumerate(whole):
        for piece in range(2):
            send_modes(table_left(fy, modes, H * piece, H), piece, send, 4 * slot)


def first_kernel(field_hbm, tabs_hbm, send, factors, tabs, field, sems):
    def load(source, target, at):
        return pltpu.make_async_copy(source, target, sems.at[at])

    own = load(field_hbm, field, 0)
    loads = [load(tabs_hbm.at[k], tabs.at[k], 1 + k) for k in range(6)]
    for one in (own, loads[FZ], loads[FY]):
        one.start()
    factor_kernel(factors)
    for one in (own, loads[FZ], loads[FY]):
        one.wait()
    for k in (FX, IX, IY, IZ):
        loads[k].start()
    pieces = [field[row, pl.ds(H * half, H), :] for row, half in PIECES]
    to_messages([pieces, [reaction(v) for v in pieces]], send, tabs.at[FZ], tabs.at[FY])
    for k in (FX, IX, IY, IZ):
        loads[k].wait()


def middle_kernel(got, tabs, send):
    pieces = from_messages(got, tabs.at[IY], tabs.at[IZ])
    to_messages([[reaction(v) for v in pieces]], send, tabs.at[FZ], tabs.at[FY])


def last_kernel(got, tabs, field_hbm, field, sems):
    stores = []
    pieces = from_messages(got, tabs.at[IY], tabs.at[IZ])
    for k, (row, half) in enumerate(PIECES):
        at = pl.ds(H * half, H)
        field[row, at, :] = pieces[k]
        one = pltpu.make_async_copy(field.at[row, at], field_hbm.at[row, at], sems.at[k])
        one.start()
        stores.append(one)
    for one in stores:
        one.wait()


def special_lane(slot, row0):
    if slot:
        return None
    device = lax.axis_index(BOTH)
    lane = piece_grid(1) + jnp.where(device == 0, 0, H) == 0
    return lane if row0 is None else lane & ~row0


def column_of(got, slot, field=0):
    at = 8 * field + 2 * slot
    column = joined(*(tile_rows(got, at + k) for k in (0, 1, 4, 5)))
    return split(column)


def modes_of(whole, slot, piece):
    cre, cim, sre, sim = quarters(whole)
    row0 = first_row(piece)
    special = special_lane(slot, row0)
    tre = pick(special, cre, pick(row0, cre, cre + sim))
    tim = pick(special, -sre, pick(row0, cim, cim - sre))
    bre = pick(special, cim, pick(row0, sre, cre - sim))
    bim = pick(special, -sim, pick(row0, sim, cim + sre))
    return tre, tim, bre, bim


PARTS = [(slot, piece) for slot in range(2) for piece in range(2)]


def spectra_of(got, fx, fields=1):
    keys = [(slot, field) for slot in range(2) for field in range(fields)]
    columns = {key: column_of(got, *key) for key in keys}
    return {
        (slot, piece): [
            modes_of(table_left(fx, columns[slot, field], H * piece, H), slot, piece)
            for field in range(fields)
        ]
        for slot, piece in PARTS
    }


def operand_of(parts, slot, piece):
    tre, tim, bre, bim = parts
    row0 = first_row(piece)
    special = special_lane(slot, row0)
    pre = pick(special, 2.0 * tre, pick(row0, tre, tre + bre))
    pim = pick(special, 2.0 * bre, pick(row0, tim, tim + bim))
    mre = pick(special, -2.0 * tim, pick(row0, bre, bim - tim))
    mim = pick(special, -2.0 * bim, pick(row0, bim, tre - bre))
    plus = split(jnp.concatenate([pre, pim], axis=1))
    minus = split(jnp.concatenate([mre, mim], axis=1))
    return plus, minus


def spectra_to(nexts, ix, send):
    sides = {key: operand_of(nexts[key], *key) for key in PARTS}
    for slot in range(2):
        one, two = sides[slot, 0], sides[slot, 1]
        operand = [
            jnp.concatenate([one[0][k], two[0][k], one[1][k], two[1][k]], axis=0) for k in range(2)
        ]
        for row in ROWS:
            out = table_left(ix, operand, H * row, H)
            put_rows(send, 4 * row + 2 * slot, out[:, :H])
            put_rows(send, 4 * row + 2 * slot + 1, out[:, H:])


def plane_of(slot, half, part):
    if slot:
        return 2 + half
    return (4 if part else 0) + half


def each_part(slot, piece):
    rows = pl.ds(Q * piece, Q)
    for half in range(2):
        for part in range(2):
            k = 2 * half + part
            yield k, (4 * slot + k, rows), (plane_of(slot, half, part), rows)


def spectral_first(got, factors, tabs, send, keep, base, total):
    spectra = spectra_of(got, tabs.at[FX], 2)
    nexts = {}
    for key in PARTS:
        state, react = spectra[key]
        nexts[key] = []
        for k, own, plane in each_part(*key):
            e_half = factors[0, *plane]
            q_half = factors[1, *plane]
            kept = e_half * state[k]
            turn = q_half * react[k]
            first = kept + turn
            keep[own] = kept
            base[own] = e_half * first - turn
            total[own] = factors[2, *plane] * state[k] + factors[3, *plane] * react[k]
            nexts[key].append(first)
    spectra_to(nexts, tabs.at[IX], send)


def spectral_middle(got, factors, kept, total, tabs, send, total_out, *, twice):
    spectra = spectra_of(got, tabs.at[FX])
    nexts = {}
    for key in PARTS:
        (react,) = spectra[key]
        nexts[key] = []
        for k, own, plane in each_part(*key):
            turn = factors[1, *plane] * react[k]
            if twice:
                turn = 2.0 * turn
            nexts[key].append(kept[own] + turn)
            total_out[own] = total[own] + 2.0 * factors[4, *plane] * react[k]
    spectra_to(nexts, tabs.at[IX], send)


def spectral_last(got, factors, total, tabs, send):
    spectra = spectra_of(got, tabs.at[FX])
    nexts = {}
    for key in PARTS:
        (react,) = spectra[key]
        nexts[key] = [
            total[own] + factors[5, *plane] * react[k] for k, own, plane in each_part(*key)
        ]
    spectra_to(nexts, tabs.at[IX], send)


def step_factors(ksq):
    lin = growth_rate - (1.0 - ksq) * (1.0 - ksq)
    z = time_step * lin
    e_half = jnp.exp(0.5 * z)
    e_full = e_half * e_half
    within = jnp.abs(z) < 1.0
    inside = jnp.where(within, z, 0.0)
    inverse = 1.0 / jnp.where(within, 2.0, z)
    series = jnp.full_like(z, 1.0 / math.factorial(14))
    for exponent in range(10, -1, -1):
        series = series * inside + 1.0 / math.factorial(exponent + 3)
    closed_one = (e_full - 1.0) * inverse
    closed_two = (closed_one - 1.0) * inverse
    third = jnp.where(within, series, (closed_two - 0.5) * inverse)
    second = jnp.where(within, 0.5 + inside * series, closed_two)
    first = jnp.where(within, 1.0 + inside * second, closed_one)
    return (
        e_half,
        time_step * first / (e_half + 1.0),
        e_full,
        time_step * (first - 3.0 * second + 4.0 * third),
        time_step * (second - 2.0 * third),
        time_step * (4.0 * third - second),
    )


def factor_kernel(factors):
    device = lax.axis_index(BOTH)
    square = H * H
    own = device * device
    alone = jnp.where(device == 0, 1, 0)

    def fill(plane, count):
        row = lax.broadcasted_iota(jnp.int32, (count, H), 0)
        lane = lax.broadcasted_iota(jnp.int32, (count, H), 1)
        half, kind = plane % 2, plane // 2
        lane0 = lane == 0
        modes = row * row
        if half:
            modes = jnp.where(row == 0, square, modes)
        if kind == 1:
            modes = modes + own + alone * square
            modes = modes + jnp.where(lane0, (1 - alone) * square, lane * lane)
        else:
            modes = modes + own + lane * lane
            pair = lane0 & (row != 0)
            if kind == 2:
                pair = lane0 if half else lane0 & (row == 0)
            if half or kind == 2:
                modes = modes + jnp.where(pair, alone * (2 * square), 0)
        values = step_factors(modes.astype(F32) * (wave_scale / N) ** 2)
        for k in range(6):
            factors[k, plane, pl.ds(0, count), :] = values[k]
            if kind == 0:
                factors[k, plane + 4, pl.ds(8, H - 8), :] = values[k][8:]

    for plane in range(4):
        fill(plane, H)
    for plane in (4, 5):
        fill(plane, 8)


def shape(*dims):
    return jax.ShapeDtypeStruct(dims, F32)


VMEM = pl.BlockSpec(memory_space=pltpu.VMEM)
HBM = pl.BlockSpec(memory_space=pltpu.HBM)


def call(kernel, outs, *args, name, ins=VMEM, into=VMEM, scratch=()):
    single = not isinstance(outs, tuple)
    return pl.pallas_call(
        kernel,
        out_shape=outs,
        in_specs=[ins] * len(args),
        out_specs=into if single else tuple(into for _ in outs),
        scratch_shapes=scratch,
        compiler_params=pltpu.CompilerParams(vmem_limit_bytes=16 << 20),
        name=name,
    )(*args)


def move(send):
    tiles = send.reshape(H, send.shape[0] // H, H)
    out = lax.all_to_all(tiles, BOTH, split_axis=0, concat_axis=0, tiled=True)
    return out.reshape(send.shape)


def body(tabs, field):
    message = shape(8 * H, H)
    spectrum = shape(8, H, H)
    send, factors, tabs = call(
        first_kernel,
        (shape(16 * H, H), shape(6, 6, H, H), jax.ShapeDtypeStruct(tabs.shape, BF16)),
        pltpu.with_memory_space_constraint(field, pltpu.HBM),
        pltpu.with_memory_space_constraint(tabs, pltpu.HBM),
        name="first",
        ins=HBM,
        scratch=[pltpu.VMEM(field.shape, F32), pltpu.SemaphoreType.DMA((7,))],
    )
    got = move(send)
    send, keep, base, total = call(
        spectral_first, (message, spectrum, spectrum, spectrum), got, factors, tabs, name="spectral_first"
    )

    def physical(send):
        return move(call(middle_kernel, message, move(send), tabs, name="physical"))

    for kept, twice in ((keep, False), (base, True)):
        got = physical(send)
        send, total = call(
            functools.partial(spectral_middle, twice=twice),
            (message, spectrum),
            got, factors, kept, total, tabs,
            name="spectral_middle",
        )
    got = physical(send)
    send = call(spectral_last, message, got, factors, total, tabs, name="spectral_last")
    return call(
        last_kernel,
        shape(*field.shape),
        move(send), tabs,
        name="last",
        into=HBM,
        scratch=[pltpu.VMEM(field.shape, F32), pltpu.SemaphoreType.DMA((4,))],
    )


def solution(mesh):
    tabs = np.stack([split_table(t) for t in tables()])
    placed = P(BOTH, None, None)

    def run(initial_field):
        return body(jnp.asarray(tabs), initial_field)

    return jax.shard_map(run, mesh=mesh, in_specs=(placed,), out_specs=placed, check_vma=False)
```

```python
import functools
import math

import jax
import jax.numpy as jnp
import numpy as np
from jax import lax
from jax.experimental import pallas as pl
from jax.experimental.pallas import tpu as pltpu
from jax.sharding import PartitionSpec as P

growth_rate = 0.3
quadratic = 1.0
time_step = 0.2
wave_scale = 4.0

N = 256
H = 128
Q = 64
BOTH = ("row", "col")
F32 = jnp.float32
BF16 = jnp.bfloat16


def tables():
    n = np.arange(N)
    j = np.arange(H)
    angle = 2.0 * np.pi / N * ((j[:, None] * n[None, :]) % N)
    cosine = np.cos(angle)
    sine = np.sin(angle)
    alternate = 1.0 - 2.0 * (n % 2)
    sine_alt = sine.copy()
    sine_alt[0] = alternate
    forward_y = np.concatenate([cosine, sine_alt])
    inverse_y = forward_y.T / N
    order = np.concatenate([np.arange(0, N, 2), np.arange(1, N, 2)])
    pieces = np.arange(N).reshape(2, 2, Q).transpose(1, 0, 2).reshape(N)
    inverse_x = inverse_y[order]
    forward_y = forward_y[pieces]
    forward_x = forward_y[:, order]
    minus = -sine
    minus[0] = alternate
    forward_z = np.concatenate([cosine, minus]).T
    weight = np.where(j == 0, 1.0, 2.0)[:, None] / N
    inverse_z = np.concatenate([cosine * weight, minus * weight])
    return forward_z, forward_y, forward_x, inverse_x, inverse_y, inverse_z


FZ, FY, FX, IX, IY, IZ = range(6)


def split_table(table):
    high = np.asarray(table, np.float32).astype(jnp.bfloat16)
    low = (table - high.astype(np.float64)).astype(np.float32).astype(jnp.bfloat16)
    return np.stack([high, low])


def split(values):
    high = values.astype(BF16)
    low = (values - high.astype(F32)).astype(BF16)
    return high, low


def dot(left, right):
    return jnp.dot(left, right, preferred_element_type=F32)


def folded(whole):
    count = whole.shape[0] // 2
    return whole[:count], whole[count:]


def table_left(table, parts, at=0, count=N):
    high, low = parts
    top, bottom = table[0, pl.ds(at, count), :], table[1, pl.ds(at, count), :]
    main, rest = folded(dot(jnp.concatenate([top, bottom], axis=0), high))
    return main + (rest + dot(top, low))


def table_right(values, table):
    high, low = split(values)
    main, rest = folded(dot(jnp.concatenate([high, low], axis=0), table[0]))
    return main + (rest + dot(high, table[1]))


def grid_of(axis):
    return lax.broadcasted_iota(jnp.int32, (H, H), axis)


def piece_grid(axis):
    return lax.broadcasted_iota(jnp.int32, (Q, H), axis)


def first_row(piece):
    return None if piece else piece_grid(0) == 0


def pick(mask, chosen, other):
    return other if mask is None else jnp.where(mask, chosen, other)


def quarters(whole):
    return whole[:Q, :H], whole[:Q, H:], whole[Q:, :H], whole[Q:, H:]


def joined(top_left, top_right, bottom_left, bottom_right):
    return jnp.concatenate(
        [
            jnp.concatenate([top_left, top_right], axis=1),
            jnp.concatenate([bottom_left, bottom_right], axis=1),
        ],
        axis=0,
    )


def tile_rows(ref, slot):
    return ref[pl.ds(slot, H, stride=ref.shape[0] // H), :]


def put_rows(ref, slot, values, at=0):
    stride = ref.shape[0] // H
    ref[pl.ds(slot + stride * at, values.shape[0], stride=stride), :] = values


def reaction(values):
    return quadratic * values * values - values * values * values


def send_modes(whole, piece, send, base):
    cre, cim, sre, sim = quarters(whole)
    lane0 = piece_grid(1) == 0
    row0 = first_row(piece)
    corner = None if row0 is None else lane0 & row0
    o0re = jnp.where(lane0 if row0 is None else lane0 | row0, cre, cre + sim)
    o0im = pick(row0, cim, jnp.where(lane0, -sre, cim - sre))
    o0im = pick(corner, sim, o0im)
    o1re = jnp.where(lane0, cim, pick(row0, sre, cre - sim))
    o1im = pick(row0, sim, jnp.where(lane0, -sim, cim + sre))
    o1im = pick(corner, sre, o1im)
    for k, values in enumerate((o0re, o0im, o1re, o1im)):
        put_rows(send, base + k, values, Q * piece)


def got_modes(got, base):
    s0re = tile_rows(got, base + 0)
    s0im = tile_rows(got, base + 1)
    s1re = tile_rows(got, base + 2)
    s1im = tile_rows(got, base + 3)
    lane0 = grid_of(1) == 0
    row0 = grid_of(0) == 0
    corner = lane0 & row0
    pre = jnp.where(lane0, 2.0 * s0re, s0re + s1re)
    pre = jnp.where(row0, s0re, pre)
    pim = jnp.where(lane0, 2.0 * s1re, s0im + s1im)
    pim = jnp.where(row0, s0im, pim)
    pim = jnp.where(corner, s1re, pim)
    mre = jnp.where(lane0, -2.0 * s0im, s1im - s0im)
    mre = jnp.where(row0, s1re, mre)
    mre = jnp.where(corner, s1im, mre)
    mim = jnp.where(lane0, -2.0 * s1im, s0re - s1re)
    mim = jnp.where(row0, s1im, mim)
    mim = jnp.where(corner, s0im, mim)
    return joined(pre, pim, mre, mim)


ROWS = range(2)
HALVES = range(2)
PIECES = [(row, half) for row in ROWS for half in HALVES]


def from_messages(got, iy, iz):
    modes = [split(got_modes(got, 4 * row)) for row in ROWS]
    parts = [table_left(iy, modes[row], H * half, H) for row, half in PIECES]
    return [table_right(part, iz) for part in parts]


def to_messages(fields, send, fz, fy):
    parts = [[table_right(piece, fz) for piece in field] for field in fields]
    whole = [
        split(jnp.concatenate(part[2 * row : 2 * row + 2], axis=0)) for part in parts for row in ROWS
    ]
    for slot, modes in enumerate(whole):
        for piece in range(2):
            send_modes(table_left(fy, modes, H * piece, H), piece, send, 4 * slot)


def first_kernel(field_hbm, tabs_hbm, send, factors, tabs, field, sems):
    def load(source, target, at):
        return pltpu.make_async_copy(source, target, sems.at[at])

    own = load(field_hbm, field, 0)
    loads = [load(tabs_hbm.at[k], tabs.at[k], 1 + k) for k in range(6)]
    for one in (own, *loads):
        one.start()
    factor_kernel(factors)
    for one in (own, loads[FZ], loads[FY]):
        one.wait()
    pieces = [field[row, pl.ds(H * half, H), :] for row, half in PIECES]
    to_messages([pieces, [reaction(v) for v in pieces]], send, tabs.at[FZ], tabs.at[FY])
    for k in (FX, IX, IY, IZ):
        loads[k].wait()


def middle_kernel(got, tabs, send):
    pieces = from_messages(got, tabs.at[IY], tabs.at[IZ])
    to_messages([[reaction(v) for v in pieces]], send, tabs.at[FZ], tabs.at[FY])


def last_kernel(got, tabs, field_hbm, field, sems):
    stores = []
    pieces = from_messages(got, tabs.at[IY], tabs.at[IZ])
    for k, (row, half) in enumerate(PIECES):
        at = pl.ds(H * half, H)
        field[row, at, :] = pieces[k]
        one = pltpu.make_async_copy(field.at[row, at], field_hbm.at[row, at], sems.at[k])
        one.start()
        stores.append(one)
    for one in stores:
        one.wait()


def special_lane(slot, row0):
    if slot:
        return None
    device = lax.axis_index(BOTH)
    lane = piece_grid(1) + jnp.where(device == 0, 0, H) == 0
    return lane if row0 is None else lane & ~row0


def column_of(got, slot, field=0):
    at = 8 * field + 2 * slot
    column = joined(*(tile_rows(got, at + k) for k in (0, 1, 4, 5)))
    return split(column)


def modes_of(whole, slot, piece):
    cre, cim, sre, sim = quarters(whole)
    row0 = first_row(piece)
    special = special_lane(slot, row0)
    tre = pick(special, cre, pick(row0, cre, cre + sim))
    tim = pick(special, -sre, pick(row0, cim, cim - sre))
    bre = pick(special, cim, pick(row0, sre, cre - sim))
    bim = pick(special, -sim, pick(row0, sim, cim + sre))
    return tre, tim, bre, bim


PARTS = [(slot, piece) for slot in range(2) for piece in range(2)]


def spectra_of(got, fx, fields=1):
    keys = [(slot, field) for slot in range(2) for field in range(fields)]
    columns = {key: column_of(got, *key) for key in keys}
    return {
        (slot, piece): [
            modes_of(table_left(fx, columns[slot, field], H * piece, H), slot, piece)
            for field in range(fields)
        ]
        for slot, piece in PARTS
    }


def operand_of(parts, slot, piece):
    tre, tim, bre, bim = parts
    row0 = first_row(piece)
    special = special_lane(slot, row0)
    pre = pick(special, 2.0 * tre, pick(row0, tre, tre + bre))
    pim = pick(special, 2.0 * bre, pick(row0, tim, tim + bim))
    mre = pick(special, -2.0 * tim, pick(row0, bre, bim - tim))
    mim = pick(special, -2.0 * bim, pick(row0, bim, tre - bre))
    plus = split(jnp.concatenate([pre, pim], axis=1))
    minus = split(jnp.concatenate([mre, mim], axis=1))
    return plus, minus


def spectra_to(nexts, ix, send):
    sides = {key: operand_of(nexts[key], *key) for key in PARTS}
    for slot in range(2):
        one, two = sides[slot, 0], sides[slot, 1]
        operand = [
            jnp.concatenate([one[0][k], two[0][k], one[1][k], two[1][k]], axis=0) for k in range(2)
        ]
        for row in ROWS:
            out = table_left(ix, operand, H * row, H)
            put_rows(send, 4 * row + 2 * slot, out[:, :H])
            put_rows(send, 4 * row + 2 * slot + 1, out[:, H:])


def plane_of(slot, half, part):
    if slot:
        return 2 + half
    return (4 if part else 0) + half


def each_part(slot, piece):
    rows = pl.ds(Q * piece, Q)
    for half in range(2):
        for part in range(2):
            k = 2 * half + part
            yield k, (4 * slot + k, rows), (plane_of(slot, half, part), rows)


def spectral_first(got, factors, tabs, send, keep, base, total):
    spectra = spectra_of(got, tabs.at[FX], 2)
    nexts = {}
    for key in PARTS:
        state, react = spectra[key]
        nexts[key] = []
        for k, own, plane in each_part(*key):
            e_half = factors[0, *plane]
            q_half = factors[1, *plane]
            kept = e_half * state[k]
            turn = q_half * react[k]
            first = kept + turn
            keep[own] = kept
            base[own] = e_half * first - turn
            total[own] = factors[2, *plane] * state[k] + factors[3, *plane] * react[k]
            nexts[key].append(first)
    spectra_to(nexts, tabs.at[IX], send)


def spectral_middle(got, factors, kept, total, tabs, send, total_out, *, twice):
    spectra = spectra_of(got, tabs.at[FX])
    nexts = {}
    for key in PARTS:
        (react,) = spectra[key]
        nexts[key] = []
        for k, own, plane in each_part(*key):
            turn = factors[1, *plane] * react[k]
            if twice:
                turn = 2.0 * turn
            nexts[key].append(kept[own] + turn)
            total_out[own] = total[own] + factors[4, *plane] * react[k]
    spectra_to(nexts, tabs.at[IX], send)


def spectral_last(got, factors, total, tabs, send):
    spectra = spectra_of(got, tabs.at[FX])
    nexts = {}
    for key in PARTS:
        (react,) = spectra[key]
        nexts[key] = [
            total[own] + factors[5, *plane] * react[k] for k, own, plane in each_part(*key)
        ]
    spectra_to(nexts, tabs.at[IX], send)


def step_factors(ksq):
    lin = growth_rate - (1.0 - ksq) * (1.0 - ksq)
    z = time_step * lin
    e_half = jnp.exp(0.5 * z)
    e_full = e_half * e_half
    within = jnp.abs(z) < 1.0
    inside = jnp.where(within, z, 0.0)
    inverse = 1.0 / jnp.where(within, 2.0, z)
    series = jnp.full_like(z, 1.0 / math.factorial(14))
    for exponent in range(10, -1, -1):
        series = series * inside + 1.0 / math.factorial(exponent + 3)
    closed_one = (e_full - 1.0) * inverse
    closed_two = (closed_one - 1.0) * inverse
    third = jnp.where(within, series, (closed_two - 0.5) * inverse)
    second = jnp.where(within, 0.5 + inside * series, closed_two)
    first = jnp.where(within, 1.0 + inside * second, closed_one)
    return (
        e_half,
        time_step * first / (e_half + 1.0),
        e_full,
        time_step * (first - 3.0 * second + 4.0 * third),
        2.0 * time_step * (second - 2.0 * third),
        time_step * (4.0 * third - second),
    )


def factor_kernel(factors):
    device = lax.axis_index(BOTH)
    square = H * H
    own = device * device
    alone = jnp.where(device == 0, 1, 0)

    def fill(plane, count):
        row = lax.broadcasted_iota(jnp.int32, (count, H), 0)
        lane = lax.broadcasted_iota(jnp.int32, (count, H), 1)
        half, kind = plane % 2, plane // 2
        lane0 = lane == 0
        modes = row * row
        if half:
            modes = jnp.where(row == 0, square, modes)
        if kind == 1:
            modes = modes + own + alone * square
            modes = modes + jnp.where(lane0, (1 - alone) * square, lane * lane)
        else:
            modes = modes + own + lane * lane
            pair = lane0 & (row != 0)
            if kind == 2:
                pair = lane0 if half else lane0 & (row == 0)
            if half or kind == 2:
                modes = modes + jnp.where(pair, alone * (2 * square), 0)
        values = step_factors(modes.astype(F32) * (wave_scale / N) ** 2)
        for k in range(6):
            factors[k, plane, pl.ds(0, count), :] = values[k]
            if kind == 0:
                factors[k, plane + 4, pl.ds(8, H - 8), :] = values[k][8:]

    for plane in range(4):
        fill(plane, H)
    for plane in (4, 5):
        fill(plane, 8)


def shape(*dims):
    return jax.ShapeDtypeStruct(dims, F32)


VMEM = pl.BlockSpec(memory_space=pltpu.VMEM)
HBM = pl.BlockSpec(memory_space=pltpu.HBM)


def call(kernel, outs, *args, name, ins=VMEM, into=VMEM, scratch=()):
    single = not isinstance(outs, tuple)
    return pl.pallas_call(
        kernel,
        out_shape=outs,
        in_specs=[ins] * len(args),
        out_specs=into if single else tuple(into for _ in outs),
        scratch_shapes=scratch,
        compiler_params=pltpu.CompilerParams(vmem_limit_bytes=16 << 20),
        name=name,
    )(*args)


def move(send):
    tiles = send.reshape(H, send.shape[0] // H, H)
    out = lax.all_to_all(tiles, BOTH, split_axis=0, concat_axis=0, tiled=True)
    return out.reshape(send.shape)


def body(tabs, field):
    message = shape(8 * H, H)
    spectrum = shape(8, H, H)
    send, factors, tabs = call(
        first_kernel,
        (shape(16 * H, H), shape(6, 6, H, H), jax.ShapeDtypeStruct(tabs.shape, BF16)),
        pltpu.with_memory_space_constraint(field, pltpu.HBM),
        pltpu.with_memory_space_constraint(tabs, pltpu.HBM),
        name="first",
        ins=HBM,
        scratch=[pltpu.VMEM(field.shape, F32), pltpu.SemaphoreType.DMA((7,))],
    )
    got = move(send)
    send, keep, base, total = call(
        spectral_first, (message, spectrum, spectrum, spectrum), got, factors, tabs, name="spectral_first"
    )

    def physical(send):
        return move(call(middle_kernel, message, move(send), tabs, name="physical"))

    for kept, twice in ((keep, False), (base, True)):
        got = physical(send)
        send, total = call(
            functools.partial(spectral_middle, twice=twice),
            (message, spectrum),
            got, factors, kept, total, tabs,
            name="spectral_middle",
        )
    got = physical(send)
    send = call(spectral_last, message, got, factors, total, tabs, name="spectral_last")
    return call(
        last_kernel,
        shape(*field.shape),
        move(send), tabs,
        name="last",
        into=HBM,
        scratch=[pltpu.VMEM(field.shape, F32), pltpu.SemaphoreType.DMA((4,))],
    )


def solution(mesh):
    tabs = np.stack([split_table(t) for t in tables()])
    placed = P(BOTH, None, None)

    def run(initial_field):
        return body(jnp.asarray(tabs), initial_field)

    return jax.shard_map(run, mesh=mesh, in_specs=(placed,), out_specs=placed, check_vma=False)
```

```python
import functools
import math

import jax
import jax.numpy as jnp
import numpy as np
from jax import lax
from jax.experimental import pallas as pl
from jax.experimental.pallas import tpu as pltpu
from jax.sharding import PartitionSpec as P

growth_rate = 0.3
quadratic = 1.0
time_step = 0.2
wave_scale = 4.0

N = 256
H = 128
Q = 64
BOTH = ("row", "col")
F32 = jnp.float32
BF16 = jnp.bfloat16


def tables():
    n = np.arange(N)
    j = np.arange(H)
    angle = 2.0 * np.pi / N * ((j[:, None] * n[None, :]) % N)
    cosine = np.cos(angle)
    sine = np.sin(angle)
    alternate = 1.0 - 2.0 * (n % 2)
    sine_alt = sine.copy()
    sine_alt[0] = alternate
    forward_y = np.concatenate([cosine, sine_alt])
    inverse_y = forward_y.T / N
    order = np.concatenate([np.arange(0, N, 2), np.arange(1, N, 2)])
    pieces = np.arange(N).reshape(2, 2, Q).transpose(1, 0, 2).reshape(N)
    inverse_x = inverse_y[order]
    forward_y = forward_y[pieces]
    forward_x = forward_y[:, order]
    minus = -sine
    minus[0] = alternate
    forward_z = np.concatenate([cosine, minus]).T
    weight = np.where(j == 0, 1.0, 2.0)[:, None] / N
    inverse_z = np.concatenate([cosine * weight, minus * weight])
    return forward_z, forward_y, forward_x, inverse_x, inverse_y, inverse_z


FZ, FY, FX, IX, IY, IZ = range(6)


def split_table(table):
    high = np.asarray(table, np.float32).astype(jnp.bfloat16)
    low = (table - high.astype(np.float64)).astype(np.float32).astype(jnp.bfloat16)
    return np.stack([high, low])


def split(values):
    high = values.astype(BF16)
    low = (values - high.astype(F32)).astype(BF16)
    return high, low


def dot(left, right):
    return jnp.dot(left, right, preferred_element_type=F32)


def folded(whole):
    count = whole.shape[0] // 2
    return whole[:count], whole[count:]


def table_left(table, parts, at=0, count=N):
    high, low = parts
    top, bottom = table[0, pl.ds(at, count), :], table[1, pl.ds(at, count), :]
    main, rest = folded(dot(jnp.concatenate([top, bottom], axis=0), high))
    return main + (rest + dot(top, low))


def table_right(values, table):
    high, low = split(values)
    main, rest = folded(dot(jnp.concatenate([high, low], axis=0), table[0]))
    return main + (rest + dot(high, table[1]))


def grid_of(axis):
    return lax.broadcasted_iota(jnp.int32, (H, H), axis)


def piece_grid(axis):
    return lax.broadcasted_iota(jnp.int32, (Q, H), axis)


def first_row(piece):
    return None if piece else piece_grid(0) == 0


def pick(mask, chosen, other):
    return other if mask is None else jnp.where(mask, chosen, other)


def quarters(whole):
    return whole[:Q, :H], whole[:Q, H:], whole[Q:, :H], whole[Q:, H:]


def joined(top_left, top_right, bottom_left, bottom_right):
    return jnp.concatenate(
        [
            jnp.concatenate([top_left, top_right], axis=1),
            jnp.concatenate([bottom_left, bottom_right], axis=1),
        ],
        axis=0,
    )


def tile_rows(ref, slot):
    return ref[pl.ds(slot, H, stride=ref.shape[0] // H), :]


def put_rows(ref, slot, values, at=0):
    stride = ref.shape[0] // H
    ref[pl.ds(slot + stride * at, values.shape[0], stride=stride), :] = values


def reaction(values):
    return values * values * (quadratic - values)


def send_modes(whole, piece, send, base):
    cre, cim, sre, sim = quarters(whole)
    lane0 = piece_grid(1) == 0
    row0 = first_row(piece)
    corner = None if row0 is None else lane0 & row0
    o0re = jnp.where(lane0 if row0 is None else lane0 | row0, cre, cre + sim)
    o0im = pick(row0, cim, jnp.where(lane0, -sre, cim - sre))
    o0im = pick(corner, sim, o0im)
    o1re = jnp.where(lane0, cim, pick(row0, sre, cre - sim))
    o1im = pick(row0, sim, jnp.where(lane0, -sim, cim + sre))
    o1im = pick(corner, sre, o1im)
    for k, values in enumerate((o0re, o0im, o1re, o1im)):
        put_rows(send, base + k, values, Q * piece)


def got_modes(got, base):
    s0re = tile_rows(got, base + 0)
    s0im = tile_rows(got, base + 1)
    s1re = tile_rows(got, base + 2)
    s1im = tile_rows(got, base + 3)
    lane0 = grid_of(1) == 0
    row0 = grid_of(0) == 0
    corner = lane0 & row0
    pre = jnp.where(lane0, 2.0 * s0re, s0re + s1re)
    pre = jnp.where(row0, s0re, pre)
    pim = jnp.where(lane0, 2.0 * s1re, s0im + s1im)
    pim = jnp.where(row0, s0im, pim)
    pim = jnp.where(corner, s1re, pim)
    mre = jnp.where(lane0, -2.0 * s0im, s1im - s0im)
    mre = jnp.where(row0, s1re, mre)
    mre = jnp.where(corner, s1im, mre)
    mim = jnp.where(lane0, -2.0 * s1im, s0re - s1re)
    mim = jnp.where(row0, s1im, mim)
    mim = jnp.where(corner, s0im, mim)
    return joined(pre, pim, mre, mim)


ROWS = range(2)
HALVES = range(2)
PIECES = [(row, half) for row in ROWS for half in HALVES]


def from_messages(got, iy, iz):
    modes = [split(got_modes(got, 4 * row)) for row in ROWS]
    parts = [table_left(iy, modes[row], H * half, H) for row, half in PIECES]
    return [table_right(part, iz) for part in parts]


def to_messages(fields, send, fz, fy):
    parts = [[table_right(piece, fz) for piece in field] for field in fields]
    whole = [
        split(jnp.concatenate(part[2 * row : 2 * row + 2], axis=0)) for part in parts for row in ROWS
    ]
    for slot, modes in enumerate(whole):
        for piece in range(2):
            send_modes(table_left(fy, modes, H * piece, H), piece, send, 4 * slot)


def first_kernel(field_hbm, tabs_hbm, send, factors, tabs, field, sems):
    def load(source, target, at):
        return pltpu.make_async_copy(source, target, sems.at[at])

    own = load(field_hbm, field, 0)
    loads = [load(tabs_hbm.at[k], tabs.at[k], 1 + k) for k in range(6)]
    for one in (own, *loads):
        one.start()
    factor_kernel(factors)
    for one in (own, loads[FZ], loads[FY]):
        one.wait()
    pieces = [field[row, pl.ds(H * half, H), :] for row, half in PIECES]
    to_messages([pieces, [reaction(v) for v in pieces]], send, tabs.at[FZ], tabs.at[FY])
    for k in (FX, IX, IY, IZ):
        loads[k].wait()


def middle_kernel(got, tabs, send):
    pieces = from_messages(got, tabs.at[IY], tabs.at[IZ])
    to_messages([[reaction(v) for v in pieces]], send, tabs.at[FZ], tabs.at[FY])


def last_kernel(got, tabs, field_hbm, field, sems):
    stores = []
    pieces = from_messages(got, tabs.at[IY], tabs.at[IZ])
    for k, (row, half) in enumerate(PIECES):
        at = pl.ds(H * half, H)
        field[row, at, :] = pieces[k]
        one = pltpu.make_async_copy(field.at[row, at], field_hbm.at[row, at], sems.at[k])
        one.start()
        stores.append(one)
    for one in stores:
        one.wait()


def special_lane(slot, row0):
    if slot:
        return None
    device = lax.axis_index(BOTH)
    lane = piece_grid(1) + jnp.where(device == 0, 0, H) == 0
    return lane if row0 is None else lane & ~row0


def column_of(got, slot, field=0):
    at = 8 * field + 2 * slot
    column = joined(*(tile_rows(got, at + k) for k in (0, 1, 4, 5)))
    return split(column)


def modes_of(whole, slot, piece):
    cre, cim, sre, sim = quarters(whole)
    row0 = first_row(piece)
    special = special_lane(slot, row0)
    tre = pick(special, cre, pick(row0, cre, cre + sim))
    tim = pick(special, -sre, pick(row0, cim, cim - sre))
    bre = pick(special, cim, pick(row0, sre, cre - sim))
    bim = pick(special, -sim, pick(row0, sim, cim + sre))
    return tre, tim, bre, bim


PARTS = [(slot, piece) for slot in range(2) for piece in range(2)]


def spectra_of(got, fx, fields=1):
    keys = [(slot, field) for slot in range(2) for field in range(fields)]
    columns = {key: column_of(got, *key) for key in keys}
    return {
        (slot, piece): [
            modes_of(table_left(fx, columns[slot, field], H * piece, H), slot, piece)
            for field in range(fields)
        ]
        for slot, piece in PARTS
    }


def operand_of(parts, slot, piece):
    tre, tim, bre, bim = parts
    row0 = first_row(piece)
    special = special_lane(slot, row0)
    pre = pick(special, 2.0 * tre, pick(row0, tre, tre + bre))
    pim = pick(special, 2.0 * bre, pick(row0, tim, tim + bim))
    mre = pick(special, -2.0 * tim, pick(row0, bre, bim - tim))
    mim = pick(special, -2.0 * bim, pick(row0, bim, tre - bre))
    plus = split(jnp.concatenate([pre, pim], axis=1))
    minus = split(jnp.concatenate([mre, mim], axis=1))
    return plus, minus


def spectra_to(nexts, ix, send):
    sides = {key: operand_of(nexts[key], *key) for key in PARTS}
    for slot in range(2):
        one, two = sides[slot, 0], sides[slot, 1]
        operand = [
            jnp.concatenate([one[0][k], two[0][k], one[1][k], two[1][k]], axis=0) for k in range(2)
        ]
        for row in ROWS:
            out = table_left(ix, operand, H * row, H)
            put_rows(send, 4 * row + 2 * slot, out[:, :H])
            put_rows(send, 4 * row + 2 * slot + 1, out[:, H:])


def plane_of(slot, half, part):
    if slot:
        return 2 + half
    return (4 if part else 0) + half


def each_part(slot, piece):
    rows = pl.ds(Q * piece, Q)
    for half in range(2):
        for part in range(2):
            k = 2 * half + part
            yield k, (4 * slot + k, rows), (plane_of(slot, half, part), rows)


def spectral_first(got, factors, tabs, send, keep, base, total):
    spectra = spectra_of(got, tabs.at[FX], 2)
    nexts = {}
    for key in PARTS:
        state, react = spectra[key]
        nexts[key] = []
        for k, own, plane in each_part(*key):
            e_half = factors[0, *plane]
            q_half = factors[1, *plane]
            kept = e_half * state[k]
            turn = q_half * react[k]
            first = kept + turn
            keep[own] = kept
            base[own] = e_half * first - turn
            total[own] = factors[2, *plane] * state[k] + factors[3, *plane] * react[k]
            nexts[key].append(first)
    spectra_to(nexts, tabs.at[IX], send)


def spectral_middle(got, factors, kept, total, tabs, send, total_out, *, twice):
    spectra = spectra_of(got, tabs.at[FX])
    nexts = {}
    for key in PARTS:
        (react,) = spectra[key]
        nexts[key] = []
        for k, own, plane in each_part(*key):
            turn = factors[1, *plane] * react[k]
            if twice:
                turn = 2.0 * turn
            nexts[key].append(kept[own] + turn)
            total_out[own] = total[own] + factors[4, *plane] * react[k]
    spectra_to(nexts, tabs.at[IX], send)


def spectral_last(got, factors, total, tabs, send):
    spectra = spectra_of(got, tabs.at[FX])
    nexts = {}
    for key in PARTS:
        (react,) = spectra[key]
        nexts[key] = [
            total[own] + factors[5, *plane] * react[k] for k, own, plane in each_part(*key)
        ]
    spectra_to(nexts, tabs.at[IX], send)


def step_factors(ksq):
    lin = growth_rate - (1.0 - ksq) * (1.0 - ksq)
    z = time_step * lin
    e_half = jnp.exp(0.5 * z)
    e_full = e_half * e_half
    within = jnp.abs(z) < 1.0
    inside = jnp.where(within, z, 0.0)
    inverse = 1.0 / jnp.where(within, 2.0, z)
    series = jnp.full_like(z, 1.0 / math.factorial(14))
    for exponent in range(10, -1, -1):
        series = series * inside + 1.0 / math.factorial(exponent + 3)
    closed_one = (e_full - 1.0) * inverse
    closed_two = (closed_one - 1.0) * inverse
    third = jnp.where(within, series, (closed_two - 0.5) * inverse)
    second = jnp.where(within, 0.5 + inside * series, closed_two)
    first = jnp.where(within, 1.0 + inside * second, closed_one)
    return (
        e_half,
        time_step * first / (e_half + 1.0),
        e_full,
        time_step * (first - 3.0 * second + 4.0 * third),
        2.0 * time_step * (second - 2.0 * third),
        time_step * (4.0 * third - second),
    )


def factor_kernel(factors):
    device = lax.axis_index(BOTH)
    square = H * H
    own = device * device
    alone = jnp.where(device == 0, 1, 0)

    def fill(plane, count):
        row = lax.broadcasted_iota(jnp.int32, (count, H), 0)
        lane = lax.broadcasted_iota(jnp.int32, (count, H), 1)
        half, kind = plane % 2, plane // 2
        lane0 = lane == 0
        modes = row * row
        if half:
            modes = jnp.where(row == 0, square, modes)
        if kind == 1:
            modes = modes + own + alone * square
            modes = modes + jnp.where(lane0, (1 - alone) * square, lane * lane)
        else:
            modes = modes + own + lane * lane
            pair = lane0 & (row != 0)
            if kind == 2:
                pair = lane0 if half else lane0 & (row == 0)
            if half or kind == 2:
                modes = modes + jnp.where(pair, alone * (2 * square), 0)
        values = step_factors(modes.astype(F32) * (wave_scale / N) ** 2)
        for k in range(6):
            factors[k, plane, pl.ds(0, count), :] = values[k]
            if kind == 0:
                factors[k, plane + 4, pl.ds(8, H - 8), :] = values[k][8:]

    for plane in range(4):
        fill(plane, H)
    for plane in (4, 5):
        fill(plane, 8)


def shape(*dims):
    return jax.ShapeDtypeStruct(dims, F32)


VMEM = pl.BlockSpec(memory_space=pltpu.VMEM)
HBM = pl.BlockSpec(memory_space=pltpu.HBM)


def call(kernel, outs, *args, name, ins=VMEM, into=VMEM, scratch=()):
    single = not isinstance(outs, tuple)
    return pl.pallas_call(
        kernel,
        out_shape=outs,
        in_specs=[ins] * len(args),
        out_specs=into if single else tuple(into for _ in outs),
        scratch_shapes=scratch,
        compiler_params=pltpu.CompilerParams(vmem_limit_bytes=16 << 20),
        name=name,
    )(*args)


def move(send):
    tiles = send.reshape(H, send.shape[0] // H, H)
    out = lax.all_to_all(tiles, BOTH, split_axis=0, concat_axis=0, tiled=True)
    return out.reshape(send.shape)


def body(tabs, field):
    message = shape(8 * H, H)
    spectrum = shape(8, H, H)
    send, factors, tabs = call(
        first_kernel,
        (shape(16 * H, H), shape(6, 6, H, H), jax.ShapeDtypeStruct(tabs.shape, BF16)),
        pltpu.with_memory_space_constraint(field, pltpu.HBM),
        pltpu.with_memory_space_constraint(tabs, pltpu.HBM),
        name="first",
        ins=HBM,
        scratch=[pltpu.VMEM(field.shape, F32), pltpu.SemaphoreType.DMA((7,))],
    )
    got = move(send)
    send, keep, base, total = call(
        spectral_first, (message, spectrum, spectrum, spectrum), got, factors, tabs, name="spectral_first"
    )

    def physical(send):
        return move(call(middle_kernel, message, move(send), tabs, name="physical"))

    for kept, twice in ((keep, False), (base, True)):
        got = physical(send)
        send, total = call(
            functools.partial(spectral_middle, twice=twice),
            (message, spectrum),
            got, factors, kept, total, tabs,
            name="spectral_middle",
        )
    got = physical(send)
    send = call(spectral_last, message, got, factors, total, tabs, name="spectral_last")
    return call(
        last_kernel,
        shape(*field.shape),
        move(send), tabs,
        name="last",
        into=HBM,
        scratch=[pltpu.VMEM(field.shape, F32), pltpu.SemaphoreType.DMA((4,))],
    )


def solution(mesh):
    tabs = np.stack([split_table(t) for t in tables()])
    placed = P(BOTH, None, None)

    def run(initial_field):
        return body(jnp.asarray(tabs), initial_field)

    return jax.shard_map(run, mesh=mesh, in_specs=(placed,), out_specs=placed, check_vma=False)
```
